256 devices in a mesh: dom: 256 (over y, x, z, core).
Axes of the slice: x: 4, y: 4, z: 8, core: 2. Of those that a mesh axis runs over, the one named last changes fastest.
Arguments:
- displacement: float32 [8, 3, 524288], P(None, None, 'dom'), may hold values from -1.5 to 1.5
- adjoint_disp: float32 [8, 3, 524288], P(None, None, 'dom'), may hold values from -1.5 to 1.5
- pressure: float32 [8, 524288], P(None, 'dom'), may hold values from -3 to 3
- adjoint_pressure: float32 [8, 524288], P(None, 'dom'), may hold values from -3 to 3
- youngs: float32 [524288], P('dom'), may hold values from 0.5 to 2
- permeability: float32 [524288], P('dom'), may hold values from 0.3 to 3
- stiffness: float32 [24, 24], replicated
- send_nodes: int32 [8, 32768], P(None, 'dom'), may hold values from 0 to 2047
- send_cells: int32 [8, 32768], P(None, 'dom'), may hold values from 0 to 2047
- elem_nodes: int32 [8, 524288], P(None, 'dom'), may hold values from 0 to 3071, as said below
- inner_faces: int32 [2, 1572864], P(None, 'dom'), may hold values from 0 to 2047
- cross_faces: int32 [2, 262144], P(None, 'dom'), may hold values from 0 to 2047, as said below
Outputs:
- grad_log_youngs: float32 [524288], P('dom')
- grad_log_perm: float32 [524288], P('dom')
The draws below stay inside these ranges and needn't reach their ends.
Inputs may be any that keep to these rules, and one draw needn't show every extreme that they name: `send_nodes`: entries refer to the partition's own nodes; block j of partition c is read by partition c - o_j, with o as in the reference program. `send_cells`: entries refer to the partition's own cells; block j of partition c is read by partition c - o_j. `elem_nodes`: local numbering as in the reference program; a ghost entry j * 128 + g always has d + o_j on the axis. The first 1536 elements of each partition name only its own nodes; corner 0 of each of the last 512 is a ghost node. `cross_faces`: row 0 is an own cell; row 1 is j * 128 + g with d + o_j always on the axis. `inner_faces`: both rows name cells of the same partition.
All inputs are finite; a program needn't handle non-finite values.
Results may differ from the reference program's by a relative error of at most 0.0003.
Values sent between devices are 32-bit elements; how exact they have to be, the bound alone decides.
No kernel may reach another device: no remote copies, remote signals or barrier semaphores. Data moves between devices by JAX's collectives and lax.ppermute only.
A program may use at most 192 MiB of HBM per device.

```python
import math
import jax
import jax.numpy as jnp
from jax import lax

EL = 2048
STEPS = 8
NB = 8
DOFS = 24
NL = 2048
EB = 512
GN = 128
GC = 128
FI = 6144
FX = 1024
NODES = 524288
CELLS = 524288
N_DOM = 256


OFFSETS = (1, -1, 2, -2, 4, -4, 8, -8)


def valid_slots(key, device):
    offsets = jnp.array(OFFSETS, dtype=jnp.int32)
    slot_id = jax.random.randint(key, device.shape, 0, NB, dtype=jnp.int32)
    target = device + offsets[slot_id]
    inside = (target >= 0) & (target < N_DOM)
    return jnp.where(inside, slot_id, slot_id ^ 1).astype(jnp.int32)


def draw_elem_nodes(key, part):
    key_list = jax.random.split(jax.random.fold_in(key, 11), 4)
    total_rows = EL * N_DOM
    device = jnp.arange(total_rows, dtype=jnp.int32) // EL
    element = jnp.arange(total_rows, dtype=jnp.int32) % EL
    own_node = jax.random.randint(key_list[0], (8, total_rows), 0, NL, dtype=jnp.int32)
    slot_id = valid_slots(key_list[1], jnp.broadcast_to(device[None, :], (8, total_rows)))
    row_id = jax.random.randint(key_list[2], (8, total_rows), 0, GN, dtype=jnp.int32)
    ghost_node = NL + slot_id * GN + row_id
    chosen = (jax.random.randint(key_list[3], (8, total_rows), 0, 2, dtype=jnp.int32) == 1) | (jnp.arange(8, dtype=jnp.int32)[:, None] == 0)
    edge_rows = element >= EL - EB
    return jnp.where(edge_rows[None, :] & chosen, ghost_node, own_node).astype(jnp.int32)


def draw_cross_faces(key, part):
    key_list = jax.random.split(jax.random.fold_in(key, 23), 3)
    total_rows = FX * N_DOM
    device = jnp.arange(total_rows, dtype=jnp.int32) // FX
    own_cell = jax.random.randint(key_list[0], (total_rows,), 0, EL, dtype=jnp.int32)
    slot_id = valid_slots(key_list[1], device)
    row_id = jax.random.randint(key_list[2], (total_rows,), 0, GC, dtype=jnp.int32)
    return jnp.stack([own_cell, slot_id * GC + row_id]).astype(jnp.int32)


def draw_stiffness(key, part):
    inner_key = jax.random.fold_in(key, 37)
    base = jax.random.normal(inner_key, (DOFS, DOFS), jnp.float32)
    return (jnp.eye(DOFS, dtype=jnp.float32) + 0.5 * (base + base.T) / math.sqrt(2.0 * DOFS)).astype(jnp.float32)


def place_ends(entries, own_key, smallest, top_value):
    place = [jax.random.randint(jax.random.fold_in(own_key, axis), (), 0, length) for axis, length in enumerate(entries.shape)]
    longest = entries.shape.index(max(entries.shape))
    neighbour = place[:longest] + [(place[longest] + 1) % entries.shape[longest]] + place[longest + 1:]
    return entries.at[tuple(place)].set(smallest).at[tuple(neighbour)].set(top_value)


def levels(stream_key, shape, pieces, least, top_value):
    gain, own = 1.0, jax.random.fold_in(stream_key, 6)
    for position, shards_of in pieces:
        draws = jnp.exp(jax.random.uniform(jax.random.fold_in(own, position), (shards_of,), jnp.float32, least / len(pieces), top_value / len(pieces)))
        gain = gain * jnp.repeat(draws, shape[position] // shards_of).reshape([-1 if axis == position else 1 for axis in range(len(shape))])
    return gain


def noise(rng, extent, deviation, bound, cuts=(), kind=jnp.bfloat16):
    values = deviation * jax.random.normal(rng, extent, jnp.float32)
    if cuts:
        values = values * levels(rng, extent, cuts, -0.22, 0.18)
    return jnp.clip(values, -bound, bound).astype(kind)


def setup_inputs(seed: int = 0) -> dict:
    splits = jax.random.split(jax.random.key(seed), 13)
    return {
        "displacement": noise(splits[0], (STEPS, 3, NODES), 0.25, 1.5, ((2, 256),), jnp.float32),
        "adjoint_disp": noise(splits[1], (STEPS, 3, NODES), 0.25, 1.5, ((2, 256),), jnp.float32),
        "pressure": noise(splits[2], (STEPS, CELLS), 0.5, 3.0, ((1, 256),), jnp.float32),
        "adjoint_pressure": noise(splits[3], (STEPS, CELLS), 0.5, 3.0, ((1, 256),), jnp.float32),
        "youngs": jnp.clip(jnp.exp(math.log(2.0) - 1.3862944 * jax.random.uniform(splits[4], (CELLS,), jnp.float32) ** levels(splits[4], (CELLS,), ((0, 256),), -0.2, 0.2)), 0.5, 2.0),
        "permeability": jnp.clip(jnp.exp(math.log(3.0) - 2.3025851 * jax.random.uniform(splits[5], (CELLS,), jnp.float32) ** levels(splits[5], (CELLS,), ((0, 256),), -0.2, 0.2)), 0.3, 3.0),
        "stiffness": draw_stiffness(jax.random.fold_in(splits[12], 71), 0),
        "send_nodes": place_ends(jax.random.randint(splits[7], (NB, GN * N_DOM), 0, NL), jax.random.fold_in(splits[7], 1), 0, NL - 1).astype(jnp.int32),
        "send_cells": place_ends(jax.random.randint(splits[8], (NB, GC * N_DOM), 0, EL), jax.random.fold_in(splits[8], 1), 0, EL - 1).astype(jnp.int32),
        "elem_nodes": draw_elem_nodes(jax.random.fold_in(splits[12], 71), 0),
        "inner_faces": place_ends(jax.random.randint(splits[10], (2, FI * N_DOM), 0, EL), jax.random.fold_in(splits[10], 1), 0, EL - 1).astype(jnp.int32),
        "cross_faces": draw_cross_faces(jax.random.fold_in(splits[12], 71), 0),
    }


OFFSETS = (1, -1, 2, -2, 4, -4, 8, -8)


def face_terms(press_a, press_b, adj_a, adj_b, perm_a, perm_b):
    product = jnp.sum((press_a - press_b) * (adj_a - adj_b), axis=0)
    denominator = (perm_a + perm_b) * (perm_a + perm_b)
    common = 2.0 * perm_a * perm_b * product / denominator
    return common * perm_b, common * perm_a


def reference(displacement, adjoint_disp, pressure, adjoint_pressure, youngs, permeability, stiffness, send_nodes, send_cells, elem_nodes, inner_faces, cross_faces):
    offsets = jnp.array(OFFSETS, dtype=jnp.int32)
    node_blocks = send_nodes.reshape(NB, N_DOM, GN)

    def one_device(device):
        sources = jnp.clip(device + offsets, 0, N_DOM - 1).astype(jnp.int32)
        ghost_nodes = node_blocks[jnp.arange(NB, dtype=jnp.int32), sources] + sources[:, None] * NL
        table = jnp.concatenate([device * NL + jnp.arange(NL, dtype=jnp.int32), ghost_nodes.reshape(-1).astype(jnp.int32)])
        connect = lax.dynamic_slice_in_dim(elem_nodes, (device * EL).astype(jnp.int32), EL, 1)
        global_nodes = table[connect]
        forward = displacement[:, :, global_nodes].reshape(STEPS, DOFS, EL)
        adjoint = adjoint_disp[:, :, global_nodes].reshape(STEPS, DOFS, EL)
        weighted = jnp.einsum("ab,tbe->tae", stiffness, forward, precision=lax.Precision.HIGHEST)
        strain = jnp.sum(adjoint * weighted, axis=(0, 1))
        modulus = lax.dynamic_slice_in_dim(youngs, (device * EL).astype(jnp.int32), EL, 0)
        return -modulus * strain

    grad_youngs = lax.map(one_device, jnp.arange(N_DOM, dtype=jnp.int32)).reshape(-1)

    inner_base = (jnp.arange(FI * N_DOM, dtype=jnp.int32) // FI) * EL
    face_a = inner_faces[0] + inner_base
    face_b = inner_faces[1] + inner_base
    cross_dev = jnp.arange(FX * N_DOM, dtype=jnp.int32) // FX
    slot_id = (cross_faces[1] // GC).astype(jnp.int32)
    row_id = (cross_faces[1] % GC).astype(jnp.int32)
    source = jnp.clip(cross_dev + offsets[slot_id], 0, N_DOM - 1).astype(jnp.int32)
    cross_a = cross_dev * EL + cross_faces[0]
    cross_b = source * EL + send_cells[slot_id, source * GC + row_id]

    term_a, term_b = face_terms(pressure[:, face_a], pressure[:, face_b], adjoint_pressure[:, face_a], adjoint_pressure[:, face_b], permeability[face_a], permeability[face_b])
    shared_a, shared_b = face_terms(pressure[:, cross_a], pressure[:, cross_b], adjoint_pressure[:, cross_a], adjoint_pressure[:, cross_b], permeability[cross_a], permeability[cross_b])
    gradient = jnp.zeros((CELLS,), jnp.float32)
    gradient = gradient.at[face_a].add(term_a).at[face_b].add(term_b)
    gradient = gradient.at[cross_a].add(shared_a).at[cross_b].add(shared_b)
    return grad_youngs, gradient
```

```python
import jax
import jax.numpy as jnp
from jax import lax
from jax.experimental import pallas as pl
from jax.experimental.pallas import tpu as pltpu
from jax.sharding import PartitionSpec as P

OFFSETS = (1, -1, 2, -2, 4, -4, 8, -8)
SLOTS = 8
STEPS = 8
EL = 2048
EB = 512
OWN = EL - EB
FI = 6144
FX = 1024
LANES = 128
OWN_CHUNKS = EL // LANES
NODE_ROWS = 6 * STEPS
FACE_ROW = NODE_ROWS + 24
FACE_K = FACE_ROW + 16 * (FX // LANES)
FACE_ID = FACE_K + 8
ROWS = FACE_ID + 8
VMEM = pltpu.CompilerParams(vmem_limit_bytes=48 * 2**20)


def lane_take(table, lo):
    return jnp.take_along_axis(table, lo, axis=1, mode="promise_in_bounds")


def split_index(row):
    wide = jnp.broadcast_to(row, (8, LANES))
    return wide & (LANES - 1), wide >> 7


def select_rows(tables, lo, hi, chunks):
    picked = [lane_take(table(0), lo) for table in tables]
    for chunk in range(1, chunks):
        here = hi == chunk
        picked = [jnp.where(here, lane_take(table(chunk), lo), old) for table, old in zip(tables, picked)]
    return picked


def select_scalar(blocks, lo, hi):
    sub = lax.broadcasted_iota(jnp.int32, (8, LANES), 0)
    total = None
    for number, block in enumerate(blocks):
        part = jnp.where(hi == sub + 8 * number, lane_take(block, lo), 0.0)
        total = part if total is None else total + part
    return jnp.sum(total, axis=0, keepdims=True)


def cell_tables(p_ref, q_ref):
    return [
        lambda h: p_ref[:, h * LANES : (h + 1) * LANES],
        lambda h: q_ref[:, h * LANES : (h + 1) * LANES],
    ]


def node_tables(d_ref, a_ref):
    def table(ref, comp):
        return lambda h: ref[comp, :, h * LANES : (h + 1) * LANES]

    return [table(d_ref, comp) for comp in range(3)] + [table(a_ref, comp) for comp in range(3)]


def face_terms(pa, qa, ka, pb, qb, kb):
    product = jnp.sum((pa - pb) * (qa - qb), axis=0, keepdims=True)
    total = ka + kb
    common = 2.0 * ka * kb * product / (total * total)
    return common * kb, common * ka


def scatter(index, term):
    length = index.shape[1]
    lo = index & (LANES - 1)
    hi = index >> 7
    hot = jnp.where(lax.broadcasted_iota(jnp.int32, (LANES, length), 0) == lo, 1.0, 0.0).astype(jnp.bfloat16)
    top = term.astype(jnp.bfloat16).astype(jnp.float32)
    rows = lax.broadcasted_iota(jnp.int32, (16, length), 0) == hi
    left = jnp.concatenate([jnp.where(rows, top, 0.0), jnp.where(rows, term - top, 0.0)], axis=0)
    out = lax.dot_general(
        left.astype(jnp.bfloat16), hot, (((1,), (1,)), ((), ())), preferred_element_type=jnp.float32
    )
    return out[:16] + out[16:]


def halves(value):
    top = value.astype(jnp.bfloat16)
    return top, (value - top.astype(jnp.float32)).astype(jnp.bfloat16)


def spread_stiffness(k_ref):
    pick = (
        lax.broadcasted_iota(jnp.int32, (192, 24), 0) // 8 == lax.broadcasted_iota(jnp.int32, (192, 24), 1)
    ).astype(jnp.float32).astype(jnp.bfloat16)
    same = (lax.broadcasted_iota(jnp.int32, (192, 192), 0) & 7) == (
        lax.broadcasted_iota(jnp.int32, (192, 192), 1) & 7
    )
    out = []
    for half in halves(k_ref[...]):
        tall = jnp.dot(pick, half, preferred_element_type=jnp.float32).astype(jnp.bfloat16)
        full = lax.dot_general(tall, pick, (((1,), (1,)), ((), ())), preferred_element_type=jnp.float32)
        out.append(jnp.where(same, full, 0.0).astype(jnp.bfloat16))
    return out


def strain_of(k_ref, f_ref, a_ref):
    top, low = spread_stiffness(k_ref)
    f_top, f_low = halves(f_ref[...])
    weighted = jnp.dot(top, f_top, preferred_element_type=jnp.float32)
    weighted += jnp.dot(low, f_top, preferred_element_type=jnp.float32)
    weighted += jnp.dot(top, f_low, preferred_element_type=jnp.float32)
    return jnp.sum(a_ref[...] * weighted, axis=0, keepdims=True)


def gather_elements(tables, chunks, elem_ref, start, f_ref, a_ref, count):
    def chunk(step, _):
        offset = pl.multiple_of(step * LANES, LANES)
        for corner in range(8):
            row = elem_ref[corner : corner + 1, pl.ds(pl.multiple_of(start + offset, LANES), LANES)]
            lo, hi = split_index(row)
            got = select_rows(tables, lo, hi, chunks)
            for comp in range(3):
                line = (8 * comp + corner) * 8
                f_ref[line : line + 8, pl.ds(offset, LANES)] = got[comp]
                a_ref[line : line + 8, pl.ds(offset, LANES)] = got[3 + comp]
        return 0

    lax.fori_loop(0, count // LANES, chunk, 0)


def pack_kernel(d_ref, a_ref, p_ref, q_ref, k_ref, sn_ref, sc_ref, cf_ref, *outs):
    send = outs[:SLOTS]
    cells_ref, faces_ref = outs[SLOTS:]
    nodes = node_tables(d_ref, a_ref)
    cells = cell_tables(p_ref, q_ref)
    perm = [k_ref[0:8, :], k_ref[8:16, :]]
    for m in range(FX // LANES):
        cols = slice(m * LANES, (m + 1) * LANES)
        lo, hi = split_index(cf_ref[0:1, cols])
        pa, qa = select_rows(cells, lo, hi, OWN_CHUNKS)
        ka = select_scalar(perm, lo, hi)
        slot = cf_ref[1:2, cols].astype(jnp.float32)
        for ref, base in [(one, FACE_ROW) for one in send] + [(faces_ref, 0)]:
            ref[base + 16 * m : base + 16 * m + 8, :] = pa
            ref[base + 16 * m + 8 : base + 16 * m + 16, :] = qa
            ref[base + 128 + m : base + 129 + m, :] = ka
            ref[base + 136 + m : base + 137 + m, :] = slot
    for j in range(SLOTS):
        lo, hi = split_index(sn_ref[j : j + 1, :])
        for number, value in enumerate(select_rows(nodes, lo, hi, OWN_CHUNKS)):
            send[j][8 * number : 8 * number + 8, :] = value
        lo, hi = split_index(sc_ref[j : j + 1, :])
        pb, qb = select_rows(cells, lo, hi, OWN_CHUNKS)
        kb = jnp.broadcast_to(select_scalar(perm, lo, hi), (8, LANES))
        for ref, base in ((send[j], NODE_ROWS), (cells_ref, 24 * j)):
            ref[base : base + 8, :] = pb
            ref[base + 8 : base + 16, :] = qb
            ref[base + 16 : base + 24, :] = kb


FACE_BLOCK = 8


def inner_kernel(d_ref, a_ref, p_ref, q_ref, k_ref, y_ref, s_ref, en_ref, if_ref, gy_ref, gp_ref, f_s, a_s, t_s):
    gather_elements(node_tables(d_ref, a_ref), OWN_CHUNKS, en_ref, 0, f_s, a_s, OWN)
    cells = cell_tables(p_ref, q_ref)
    perm = [k_ref[0:8, :], k_ref[8:16, :]]

    def block(step, _):
        for m in range(FACE_BLOCK):
            offset = pl.multiple_of(step * (FACE_BLOCK * LANES) + m * LANES, LANES)
            ends = []
            for side in range(2):
                lo, hi = split_index(if_ref[side : side + 1, pl.ds(offset, LANES)])
                ends += select_rows(cells, lo, hi, OWN_CHUNKS) + [select_scalar(perm, lo, hi)]
            term_a, term_b = face_terms(*ends)
            t_s[0:1, pl.ds(offset, LANES)] = term_a
            t_s[1:2, pl.ds(offset, LANES)] = term_b
        return 0

    lax.fori_loop(0, FI // (FACE_BLOCK * LANES), block, 0)

    def add(step, total):
        cols = pl.ds(pl.multiple_of(step * 1024, 1024), 1024)
        for side in range(2):
            total = total + scatter(if_ref[side : side + 1, cols], t_s[side : side + 1, cols])
        return total

    gp_ref[...] = lax.fori_loop(0, FI // 1024, add, jnp.zeros((16, LANES), jnp.float32))
    gy_ref[...] = -y_ref[:, :OWN] * strain_of(s_ref, f_s, a_s)


def tail_kernel(*refs):
    got = refs[:SLOTS]
    (d_ref, a_ref, cells_ref, faces_ref, y_ref, s_ref, sc_ref, en_ref, cf_ref, gyi_ref, gpi_ref) = refs[SLOTS : SLOTS + 11]
    gy_ref, gp_ref, f_s, a_s, i_s, t_s = refs[SLOTS + 11 :]

    own = node_tables(d_ref, a_ref)

    def table(number):
        def read(h):
            if h < OWN_CHUNKS:
                return own[number](h)
            return got[h - OWN_CHUNKS][8 * number : 8 * number + 8, :]

        return read

    gather_elements([table(number) for number in range(6)], OWN_CHUNKS + SLOTS, en_ref, OWN, f_s, a_s, EB)

    ghosts = [
        lambda h: got[h][NODE_ROWS : NODE_ROWS + 8, :],
        lambda h: got[h][NODE_ROWS + 8 : NODE_ROWS + 16, :],
    ]
    ghost_perm = jnp.concatenate([got[j][NODE_ROWS + 16 : NODE_ROWS + 17, :] for j in range(SLOTS)], axis=0)
    for m in range(FX // LANES):
        cols = slice(m * LANES, (m + 1) * LANES)
        lo, hi = split_index(cf_ref[1:2, cols])
        pb, qb = select_rows(ghosts, lo, hi, SLOTS)
        kb = select_scalar([ghost_perm], lo, hi)
        pa = faces_ref[16 * m : 16 * m + 8, :]
        qa = faces_ref[16 * m + 8 : 16 * m + 16, :]
        ka = faces_ref[128 + m : 129 + m, :]
        i_s[0:1, cols] = cf_ref[0:1, cols]
        t_s[0:1, cols] = face_terms(pa, qa, ka, pb, qb, kb)[0]
    for j in range(SLOTS):
        mine = j ^ 1
        pt = cells_ref[24 * mine : 24 * mine + 8, :]
        qt = cells_ref[24 * mine + 8 : 24 * mine + 16, :]
        kt = cells_ref[24 * mine + 16 : 24 * mine + 24, :]
        place = jnp.broadcast_to(sc_ref[mine : mine + 1, :], (8, LANES))
        for m in range(FX // LANES):
            cols = slice((j + 1) * FX + m * LANES, (j + 1) * FX + (m + 1) * LANES)
            lo, hi = split_index(got[j][FACE_ID + m : FACE_ID + m + 1, :].astype(jnp.int32))
            pa = got[j][FACE_ROW + 16 * m : FACE_ROW + 16 * m + 8, :]
            qa = got[j][FACE_ROW + 16 * m + 8 : FACE_ROW + 16 * m + 16, :]
            ka = got[j][FACE_K + m : FACE_K + m + 1, :]
            kb = lane_take(kt, lo)[0:1]
            term = face_terms(pa, qa, ka, lane_take(pt, lo), lane_take(qt, lo), kb)[1]
            i_s[0:1, cols] = lane_take(place, lo)[0:1]
            t_s[0:1, cols] = jnp.where(hi[0:1] == mine, term, 0.0)

    def add(step, total):
        cols = pl.ds(pl.multiple_of(step * 1024, 1024), 1024)
        return total + scatter(i_s[0:1, cols], t_s[0:1, cols])

    gp_ref[...] = lax.fori_loop(0, SLOTS + 1, add, gpi_ref[...])
    gy_ref[:, :OWN] = gyi_ref[...]
    gy_ref[:, OWN:] = -y_ref[:, OWN:] * strain_of(s_ref, f_s, a_s)


def shape(*dims):
    return jax.ShapeDtypeStruct(dims, jnp.float32)


def on_device(
    displacement,
    adjoint_disp,
    pressure,
    adjoint_pressure,
    youngs,
    permeability,
    stiffness,
    send_nodes,
    send_cells,
    elem_nodes,
    inner_faces,
    cross_faces,
):
    forward = displacement.transpose(1, 0, 2)
    adjoint = adjoint_disp.transpose(1, 0, 2)
    perm = permeability.reshape(OWN_CHUNKS, LANES)
    young = youngs.reshape(1, EL)
    packed = pl.pallas_call(
        pack_kernel,
        out_shape=[shape(ROWS, LANES)] * SLOTS + [shape(24 * SLOTS, LANES), shape(144, LANES)],
        compiler_params=VMEM,
        name="pack",
    )(forward, adjoint, pressure, adjoint_pressure, perm, send_nodes, send_cells, cross_faces)
    cells, faces = packed[SLOTS:]
    count = lax.axis_size("dom")
    got = [
        lax.ppermute(packed[j], "dom", [(source, (source - step) % count) for source in range(count)])
        for j, step in enumerate(OFFSETS)
    ]
    inner_young, inner_perm = pl.pallas_call(
        inner_kernel,
        out_shape=[shape(1, OWN), shape(OWN_CHUNKS, LANES)],
        scratch_shapes=[
            pltpu.VMEM((192, OWN), jnp.float32),
            pltpu.VMEM((192, OWN), jnp.float32),
            pltpu.VMEM((2, FI), jnp.float32),
        ],
        compiler_params=VMEM,
        cost_estimate=pl.CostEstimate(flops=4 * 10**9, bytes_accessed=10**7, transcendentals=0),
        name="inner",
    )(forward, adjoint, pressure, adjoint_pressure, perm, young, stiffness, elem_nodes, inner_faces)
    grad_young, grad_perm = pl.pallas_call(
        tail_kernel,
        out_shape=[shape(1, EL), shape(OWN_CHUNKS, LANES)],
        scratch_shapes=[
            pltpu.VMEM((192, EB), jnp.float32),
            pltpu.VMEM((192, EB), jnp.float32),
            pltpu.VMEM((1, (SLOTS + 1) * FX), jnp.int32),
            pltpu.VMEM((1, (SLOTS + 1) * FX), jnp.float32),
        ],
        compiler_params=VMEM,
        name="tail",
    )(*got, forward, adjoint, cells, faces, young, stiffness, send_cells, elem_nodes, cross_faces, inner_young, inner_perm)
    return (grad_young.reshape(EL), grad_perm.reshape(EL))


def solution(mesh):
    in_specs = (
        P(None, None, "dom"),
        P(None, None, "dom"),
        P(None, "dom"),
        P(None, "dom"),
        P("dom"),
        P("dom"),
        P(),
        P(None, "dom"),
        P(None, "dom"),
        P(None, "dom"),
        P(None, "dom"),
        P(None, "dom"),
    )
    out_specs = (P("dom"), P("dom"))
    return jax.shard_map(
        on_device, mesh=mesh, in_specs=in_specs, out_specs=out_specs, check_vma=False
    )
```

```python
import jax
import jax.numpy as jnp
from jax import lax
from jax.experimental import pallas as pl
from jax.experimental.pallas import tpu as pltpu
from jax.sharding import PartitionSpec as P

OFFSETS = (1, -1, 2, -2, 4, -4, 8, -8)
SLOTS = 8
STEPS = 8
EL = 2048
EB = 512
OWN = EL - EB
FI = 6144
FX = 1024
LANES = 128
OWN_CHUNKS = EL // LANES
NODE_ROWS = 6 * STEPS
FACE_ROW = NODE_ROWS + 24
FACE_K = FACE_ROW + 16 * (FX // LANES)
FACE_ID = FACE_K + 8
ROWS = FACE_ID + 8
VMEM = pltpu.CompilerParams(vmem_limit_bytes=48 * 2**20)


def lane_take(table, lo):
    return jnp.take_along_axis(table, lo, axis=1, mode="promise_in_bounds")


def split_index(row):
    wide = jnp.broadcast_to(row, (8, LANES))
    return wide & (LANES - 1), wide >> 7


def select_rows(tables, lo, hi, chunks):
    picked = [lane_take(table(0), lo) for table in tables]
    for chunk in range(1, chunks):
        here = hi == chunk
        picked = [jnp.where(here, lane_take(table(chunk), lo), old) for table, old in zip(tables, picked)]
    return picked


def select_scalar(blocks, lo, hi):
    sub = lax.broadcasted_iota(jnp.int32, (8, LANES), 0)
    total = None
    for number, block in enumerate(blocks):
        part = jnp.where(hi == sub + 8 * number, lane_take(block, lo), 0.0)
        total = part if total is None else total + part
    return jnp.sum(total, axis=0, keepdims=True)


def cell_tables(p_ref, q_ref):
    return [
        lambda h: p_ref[:, h * LANES : (h + 1) * LANES],
        lambda h: q_ref[:, h * LANES : (h + 1) * LANES],
    ]


def node_tables(d_ref, a_ref):
    def table(ref, comp):
        return lambda h: ref[comp, :, h * LANES : (h + 1) * LANES]

    return [table(d_ref, comp) for comp in range(3)] + [table(a_ref, comp) for comp in range(3)]


def face_terms(pa, qa, ka, pb, qb, kb):
    product = jnp.sum((pa - pb) * (qa - qb), axis=0, keepdims=True)
    total = ka + kb
    common = 2.0 * ka * kb * product / (total * total)
    return common * kb, common * ka


def scatter(index, term):
    length = index.shape[1]
    lo = index & (LANES - 1)
    hi = index >> 7
    hot = jnp.where(lax.broadcasted_iota(jnp.int32, (LANES, length), 0) == lo, 1.0, 0.0).astype(jnp.bfloat16)
    top = term.astype(jnp.bfloat16).astype(jnp.float32)
    rows = lax.broadcasted_iota(jnp.int32, (16, length), 0) == hi
    left = jnp.concatenate([jnp.where(rows, top, 0.0), jnp.where(rows, term - top, 0.0)], axis=0)
    out = lax.dot_general(
        left.astype(jnp.bfloat16), hot, (((1,), (1,)), ((), ())), preferred_element_type=jnp.float32
    )
    return out[:16] + out[16:]


def halves(value):
    top = value.astype(jnp.bfloat16)
    return top, (value - top.astype(jnp.float32)).astype(jnp.bfloat16)


def spread_stiffness(k_ref):
    pick = (
        lax.broadcasted_iota(jnp.int32, (192, 24), 0) // 8 == lax.broadcasted_iota(jnp.int32, (192, 24), 1)
    ).astype(jnp.float32).astype(jnp.bfloat16)
    same = (lax.broadcasted_iota(jnp.int32, (192, 192), 0) & 7) == (
        lax.broadcasted_iota(jnp.int32, (192, 192), 1) & 7
    )
    out = []
    for half in halves(k_ref[...]):
        tall = jnp.dot(pick, half, preferred_element_type=jnp.float32).astype(jnp.bfloat16)
        full = lax.dot_general(tall, pick, (((1,), (1,)), ((), ())), preferred_element_type=jnp.float32)
        out.append(jnp.where(same, full, 0.0).astype(jnp.bfloat16))
    return out


def strain_of(k_ref, f_ref, a_ref):
    top, low = spread_stiffness(k_ref)
    f_top, f_low = halves(f_ref[...])
    weighted = jnp.dot(top, f_top, preferred_element_type=jnp.float32)
    weighted += jnp.dot(low, f_top, preferred_element_type=jnp.float32)
    weighted += jnp.dot(top, f_low, preferred_element_type=jnp.float32)
    return jnp.sum(a_ref[...] * weighted, axis=0, keepdims=True)


def gather_elements(tables, chunks, elem_ref, start, f_ref, a_ref, count):
    def chunk(step, _):
        offset = pl.multiple_of(step * LANES, LANES)
        for corner in range(8):
            row = elem_ref[corner : corner + 1, pl.ds(pl.multiple_of(start + offset, LANES), LANES)]
            lo, hi = split_index(row)
            got = select_rows(tables, lo, hi, chunks)
            for comp in range(3):
                line = (8 * comp + corner) * 8
                f_ref[line : line + 8, pl.ds(offset, LANES)] = got[comp]
                a_ref[line : line + 8, pl.ds(offset, LANES)] = got[3 + comp]
        return 0

    lax.fori_loop(0, count // LANES, chunk, 0)


def pack_kernel(*refs):
    sources, outs, local, sem = refs[:8], refs[8 : 10 + SLOTS], refs[10 + SLOTS : 18 + SLOTS], refs[-1]
    send = [outs[ORDER.index(j)] for j in range(SLOTS)]
    cells_ref, faces_ref = outs[SLOTS:]
    copies = [pltpu.make_async_copy(far, near, sem.at[n]) for n, (far, near) in enumerate(zip(sources, local))]
    for copy in copies:
        copy.start()
    for copy in copies:
        copy.wait()
    d_ref, a_ref, p_ref, q_ref, k_ref, sn_ref, sc_ref, cf_ref = local
    nodes = node_tables(d_ref, a_ref)
    cells = cell_tables(p_ref, q_ref)
    perm = [k_ref[0:8, :], k_ref[8:16, :]]
    for m in range(FX // LANES):
        cols = slice(m * LANES, (m + 1) * LANES)
        lo, hi = split_index(cf_ref[0:1, cols])
        pa, qa = select_rows(cells, lo, hi, OWN_CHUNKS)
        ka = select_scalar(perm, lo, hi)
        slot = cf_ref[1:2, cols].astype(jnp.float32)
        for ref, base in [(one, FACE_ROW) for one in send] + [(faces_ref, 0)]:
            ref[base + 16 * m : base + 16 * m + 8, :] = pa
            ref[base + 16 * m + 8 : base + 16 * m + 16, :] = qa
            ref[base + 128 + m : base + 129 + m, :] = ka
            ref[base + 136 + m : base + 137 + m, :] = slot
    for j in range(SLOTS):
        lo, hi = split_index(sn_ref[j : j + 1, :])
        for number, value in enumerate(select_rows(nodes, lo, hi, OWN_CHUNKS)):
            send[j][8 * number : 8 * number + 8, :] = value
        lo, hi = split_index(sc_ref[j : j + 1, :])
        pb, qb = select_rows(cells, lo, hi, OWN_CHUNKS)
        kb = jnp.broadcast_to(select_scalar(perm, lo, hi), (8, LANES))
        for ref, base in ((send[j], NODE_ROWS), (cells_ref, 24 * j)):
            ref[base : base + 8, :] = pb
            ref[base + 8 : base + 16, :] = qb
            ref[base + 16 : base + 24, :] = kb


FACE_BLOCK = 8
ORDER = (6, 4, 2, 0, 7, 1, 5, 3)


def inner_kernel(d_ref, a_ref, p_ref, q_ref, k_ref, y_ref, s_ref, en_ref, if_ref, gy_ref, gp_ref, f_s, a_s, t_s):
    gather_elements(node_tables(d_ref, a_ref), OWN_CHUNKS, en_ref, 0, f_s, a_s, OWN)
    cells = cell_tables(p_ref, q_ref)
    perm = [k_ref[0:8, :], k_ref[8:16, :]]

    def block(step, _):
        for m in range(FACE_BLOCK):
            offset = pl.multiple_of(step * (FACE_BLOCK * LANES) + m * LANES, LANES)
            ends = []
            for side in range(2):
                lo, hi = split_index(if_ref[side : side + 1, pl.ds(offset, LANES)])
                ends += select_rows(cells, lo, hi, OWN_CHUNKS) + [select_scalar(perm, lo, hi)]
            term_a, term_b = face_terms(*ends)
            t_s[0:1, pl.ds(offset, LANES)] = term_a
            t_s[1:2, pl.ds(offset, LANES)] = term_b
        return 0

    lax.fori_loop(0, FI // (FACE_BLOCK * LANES), block, 0)

    def add(step, total):
        cols = pl.ds(pl.multiple_of(step * 1024, 1024), 1024)
        for side in range(2):
            total = total + scatter(if_ref[side : side + 1, cols], t_s[side : side + 1, cols])
        return total

    gp_ref[...] = lax.fori_loop(0, FI // 1024, add, jnp.zeros((16, LANES), jnp.float32))
    gy_ref[...] = -y_ref[:, :OWN] * strain_of(s_ref, f_s, a_s)


def tail_kernel(*refs):
    got = [refs[ORDER.index(j)] for j in range(SLOTS)]
    (d_ref, a_ref, cells_ref, faces_ref, y_ref, s_ref, sc_ref, en_ref, cf_ref, gyi_ref, gpi_ref) = refs[SLOTS : SLOTS + 11]
    gy_ref, gp_ref, f_s, a_s, i_s, t_s = refs[SLOTS + 11 :]

    own = node_tables(d_ref, a_ref)

    def table(number):
        def read(h):
            if h < OWN_CHUNKS:
                return own[number](h)
            return got[h - OWN_CHUNKS][8 * number : 8 * number + 8, :]

        return read

    gather_elements([table(number) for number in range(6)], OWN_CHUNKS + SLOTS, en_ref, OWN, f_s, a_s, EB)

    ghosts = [
        lambda h: got[h][NODE_ROWS : NODE_ROWS + 8, :],
        lambda h: got[h][NODE_ROWS + 8 : NODE_ROWS + 16, :],
    ]
    ghost_perm = jnp.concatenate([got[j][NODE_ROWS + 16 : NODE_ROWS + 17, :] for j in range(SLOTS)], axis=0)
    for m in range(FX // LANES):
        cols = slice(m * LANES, (m + 1) * LANES)
        lo, hi = split_index(cf_ref[1:2, cols])
        pb, qb = select_rows(ghosts, lo, hi, SLOTS)
        kb = select_scalar([ghost_perm], lo, hi)
        pa = faces_ref[16 * m : 16 * m + 8, :]
        qa = faces_ref[16 * m + 8 : 16 * m + 16, :]
        ka = faces_ref[128 + m : 129 + m, :]
        i_s[0:1, cols] = cf_ref[0:1, cols]
        t_s[0:1, cols] = face_terms(pa, qa, ka, pb, qb, kb)[0]
    for j in range(SLOTS):
        mine = j ^ 1
        pt = cells_ref[24 * mine : 24 * mine + 8, :]
        qt = cells_ref[24 * mine + 8 : 24 * mine + 16, :]
        kt = cells_ref[24 * mine + 16 : 24 * mine + 24, :]
        place = jnp.broadcast_to(sc_ref[mine : mine + 1, :], (8, LANES))
        for m in range(FX // LANES):
            cols = slice((j + 1) * FX + m * LANES, (j + 1) * FX + (m + 1) * LANES)
            lo, hi = split_index(got[j][FACE_ID + m : FACE_ID + m + 1, :].astype(jnp.int32))
            pa = got[j][FACE_ROW + 16 * m : FACE_ROW + 16 * m + 8, :]
            qa = got[j][FACE_ROW + 16 * m + 8 : FACE_ROW + 16 * m + 16, :]
            ka = got[j][FACE_K + m : FACE_K + m + 1, :]
            kb = lane_take(kt, lo)[0:1]
            term = face_terms(pa, qa, ka, lane_take(pt, lo), lane_take(qt, lo), kb)[1]
            i_s[0:1, cols] = lane_take(place, lo)[0:1]
            t_s[0:1, cols] = jnp.where(hi[0:1] == mine, term, 0.0)

    def add(step, total):
        cols = pl.ds(pl.multiple_of(step * 1024, 1024), 1024)
        return total + scatter(i_s[0:1, cols], t_s[0:1, cols])

    gp_ref[...] = lax.fori_loop(0, SLOTS + 1, add, gpi_ref[...])
    gy_ref[:, :OWN] = gyi_ref[...]
    gy_ref[:, OWN:] = -y_ref[:, OWN:] * strain_of(s_ref, f_s, a_s)


def shape(*dims):
    return jax.ShapeDtypeStruct(dims, jnp.float32)


def on_device(
    displacement,
    adjoint_disp,
    pressure,
    adjoint_pressure,
    youngs,
    permeability,
    stiffness,
    send_nodes,
    send_cells,
    elem_nodes,
    inner_faces,
    cross_faces,
):
    forward = displacement.transpose(1, 0, 2)
    adjoint = adjoint_disp.transpose(1, 0, 2)
    perm = permeability.reshape(OWN_CHUNKS, LANES)
    young = youngs.reshape(1, EL)
    sources = (forward, adjoint, pressure, adjoint_pressure, perm, send_nodes, send_cells, cross_faces)
    packed = pl.pallas_call(
        pack_kernel,
        out_shape=[shape(ROWS, LANES)] * SLOTS + [shape(24 * SLOTS, LANES), shape(144, LANES)],
        in_specs=[pl.BlockSpec(memory_space=pltpu.HBM)] * 8,
        scratch_shapes=[
            pltpu.VMEM((3, STEPS, EL), jnp.float32),
            pltpu.VMEM((3, STEPS, EL), jnp.float32),
            pltpu.VMEM((STEPS, EL), jnp.float32),
            pltpu.VMEM((STEPS, EL), jnp.float32),
            pltpu.VMEM((OWN_CHUNKS, LANES), jnp.float32),
            pltpu.VMEM((SLOTS, LANES), jnp.int32),
            pltpu.VMEM((SLOTS, LANES), jnp.int32),
            pltpu.VMEM((2, FX), jnp.int32),
            pltpu.SemaphoreType.DMA((8,)),
        ],
        compiler_params=VMEM,
        name="pack",
    )(*(pltpu.with_memory_space_constraint(one, pltpu.HBM) for one in sources))
    cells, faces = packed[SLOTS:]
    count = lax.axis_size("dom")
    got = [
        lax.ppermute(block, "dom", [(source, (source - OFFSETS[j]) % count) for source in range(count)])
        for j, block in zip(ORDER, packed)
    ]
    inner_young, inner_perm = pl.pallas_call(
        inner_kernel,
        out_shape=[shape(1, OWN), shape(OWN_CHUNKS, LANES)],
        scratch_shapes=[
            pltpu.VMEM((192, OWN), jnp.float32),
            pltpu.VMEM((192, OWN), jnp.float32),
            pltpu.VMEM((2, FI), jnp.float32),
        ],
        compiler_params=VMEM,
        cost_estimate=pl.CostEstimate(flops=4 * 10**9, bytes_accessed=10**7, transcendentals=0),
        name="inner",
    )(forward, adjoint, pressure, adjoint_pressure, perm, young, stiffness, elem_nodes, inner_faces)
    grad_young, grad_perm = pl.pallas_call(
        tail_kernel,
        out_shape=[shape(1, EL), shape(OWN_CHUNKS, LANES)],
        scratch_shapes=[
            pltpu.VMEM((192, EB), jnp.float32),
            pltpu.VMEM((192, EB), jnp.float32),
            pltpu.VMEM((1, (SLOTS + 1) * FX), jnp.int32),
            pltpu.VMEM((1, (SLOTS + 1) * FX), jnp.float32),
        ],
        compiler_params=VMEM,
        name="tail",
    )(*got, forward, adjoint, cells, faces, young, stiffness, send_cells, elem_nodes, cross_faces, inner_young, inner_perm)
    return (grad_young.reshape(EL), grad_perm.reshape(EL))


def solution(mesh):
    in_specs = (
        P(None, None, "dom"),
        P(None, None, "dom"),
        P(None, "dom"),
        P(None, "dom"),
        P("dom"),
        P("dom"),
        P(),
        P(None, "dom"),
        P(None, "dom"),
        P(None, "dom"),
        P(None, "dom"),
        P(None, "dom"),
    )
    out_specs = (P("dom"), P("dom"))
    return jax.shard_map(
        on_device, mesh=mesh, in_specs=in_specs, out_specs=out_specs, check_vma=False
    )
```

```python
import jax
import jax.numpy as jnp
from jax import lax
from jax.experimental import pallas as pl
from jax.experimental.pallas import tpu as pltpu
from jax.sharding import PartitionSpec as P

OFFSETS = (1, -1, 2, -2, 4, -4, 8, -8)
SLOTS = 8
STEPS = 8
EL = 2048
EB = 512
OWN = EL - EB
FI = 6144
FX = 1024
LANES = 128
OWN_CHUNKS = EL // LANES
NODE_ROWS = 6 * STEPS
FACE_ROW = NODE_ROWS + 24
FACE_K = FACE_ROW + 16 * (FX // LANES)
FACE_ID = FACE_K + 8
ROWS = FACE_ID + 8
VMEM = pltpu.CompilerParams(vmem_limit_bytes=48 * 2**20)


def lane_take(table, lo):
    return jnp.take_along_axis(table, lo, axis=1, mode="promise_in_bounds")


def split_index(row):
    wide = jnp.broadcast_to(row, (8, LANES))
    return wide & (LANES - 1), wide >> 7


def select_rows(tables, lo, hi, chunks):
    picked = [lane_take(table(0), lo) for table in tables]
    for chunk in range(1, chunks):
        here = hi == chunk
        picked = [jnp.where(here, lane_take(table(chunk), lo), old) for table, old in zip(tables, picked)]
    return picked


def select_scalar(blocks, lo, hi):
    sub = lax.broadcasted_iota(jnp.int32, (8, LANES), 0)
    total = None
    for number, block in enumerate(blocks):
        part = jnp.where(hi == sub + 8 * number, lane_take(block, lo), 0.0)
        total = part if total is None else total + part
    return jnp.sum(total, axis=0, keepdims=True)


def cell_tables(p_ref, q_ref):
    return [
        lambda h: p_ref[:, h * LANES : (h + 1) * LANES],
        lambda h: q_ref[:, h * LANES : (h + 1) * LANES],
    ]


def node_tables(d_ref, a_ref):
    def table(ref, comp):
        return lambda h: ref[comp, :, h * LANES : (h + 1) * LANES]

    return [table(d_ref, comp) for comp in range(3)] + [table(a_ref, comp) for comp in range(3)]


def face_terms(pa, qa, ka, pb, qb, kb):
    product = jnp.sum((pa - pb) * (qa - qb), axis=0, keepdims=True)
    total = ka + kb
    common = 2.0 * ka * kb * product / (total * total)
    return common * kb, common * ka


def scatter(index, term):
    length = index.shape[1]
    lo = index & (LANES - 1)
    hi = index >> 7
    hot = jnp.where(lax.broadcasted_iota(jnp.int32, (LANES, length), 0) == lo, 1.0, 0.0).astype(jnp.bfloat16)
    top = term.astype(jnp.bfloat16).astype(jnp.float32)
    rows = lax.broadcasted_iota(jnp.int32, (16, length), 0) == hi
    left = jnp.concatenate([jnp.where(rows, top, 0.0), jnp.where(rows, term - top, 0.0)], axis=0)
    out = lax.dot_general(
        left.astype(jnp.bfloat16), hot, (((1,), (1,)), ((), ())), preferred_element_type=jnp.float32
    )
    return out[:16] + out[16:]


def halves(value):
    top = value.astype(jnp.bfloat16)
    return top, (value - top.astype(jnp.float32)).astype(jnp.bfloat16)


def spread_stiffness(k_ref):
    pick = (
        lax.broadcasted_iota(jnp.int32, (192, 24), 0) // 8 == lax.broadcasted_iota(jnp.int32, (192, 24), 1)
    ).astype(jnp.float32).astype(jnp.bfloat16)
    same = (lax.broadcasted_iota(jnp.int32, (192, 192), 0) & 7) == (
        lax.broadcasted_iota(jnp.int32, (192, 192), 1) & 7
    )
    out = []
    for half in halves(k_ref[...]):
        tall = jnp.dot(pick, half, preferred_element_type=jnp.float32).astype(jnp.bfloat16)
        full = lax.dot_general(tall, pick, (((1,), (1,)), ((), ())), preferred_element_type=jnp.float32)
        out.append(jnp.where(same, full, 0.0).astype(jnp.bfloat16))
    return out


def strain_of(k_ref, f_ref, a_ref):
    top, low = spread_stiffness(k_ref)
    f_top, f_low = halves(f_ref[...])
    weighted = jnp.dot(top, f_top, preferred_element_type=jnp.float32)
    weighted += jnp.dot(low, f_top, preferred_element_type=jnp.float32)
    weighted += jnp.dot(top, f_low, preferred_element_type=jnp.float32)
    return jnp.sum(a_ref[...] * weighted, axis=0, keepdims=True)


def fill_table(raw_ref, tab_ref, chunks, read):
    for chunk in range(chunks):
        for number in range(6):
            line = 48 * chunk + 8 * number
            raw_ref[line : line + 8, :] = read(number, chunk)
    top, low = halves(raw_ref[...])
    tab_ref[:, :LANES] = top
    tab_ref[:, LANES:] = low


def gather_pair(tab_ref, elem, corners, first, last, f_ref, a_ref, cols):
    sub = lax.broadcasted_iota(jnp.int32, (LANES, LANES), 0)
    hot = jnp.concatenate(
        [jnp.where(sub == (elem[n : n + 1] & (LANES - 1)), 1.0, 0.0).astype(jnp.bfloat16) for n in corners], axis=1
    )
    found = jnp.dot(
        tab_ref[48 * first : 48 * last, :],
        jnp.concatenate([hot, hot], axis=0),
        preferred_element_type=jnp.float32,
    )
    for place, corner in enumerate(corners):
        hi = jnp.broadcast_to(elem[corner : corner + 1] >> 7, (8, LANES))
        got = [found[8 * r : 8 * r + 8, place * LANES : (place + 1) * LANES] for r in range(6)]
        for chunk in range(first + 1, last):
            here = hi == chunk
            base = 48 * (chunk - first)
            got = [
                jnp.where(here, found[base + 8 * r : base + 8 * r + 8, place * LANES : (place + 1) * LANES], old)
                for r, old in enumerate(got)
            ]
        for comp in range(3):
            line = (8 * comp + corner) * 8
            f_ref[line : line + 8, cols] = got[comp]
            a_ref[line : line + 8, cols] = got[3 + comp]


SOURCES = 12


def pack_kernel(*refs):
    sources, outs, sem = refs[:SOURCES], refs[SOURCES:-1], refs[-1]
    local = outs[SLOTS + 2 :]
    send = [outs[ORDER.index(j)] for j in range(SLOTS)]
    cells_ref, faces_ref = outs[SLOTS : SLOTS + 2]
    copies = [pltpu.make_async_copy(far, near, sem.at[n]) for n, (far, near) in enumerate(zip(sources, local))]
    for copy in copies:
        copy.start()
    for copy in copies[:8]:
        copy.wait()
    p_ref, q_ref, k_ref, cf_ref, sc_ref, sn_ref, d_ref, a_ref = local[:8]
    nodes = node_tables(d_ref, a_ref)
    cells = cell_tables(p_ref, q_ref)
    perm = [k_ref[0:8, :], k_ref[8:16, :]]
    for m in range(FX // LANES):
        cols = slice(m * LANES, (m + 1) * LANES)
        lo, hi = split_index(cf_ref[0:1, cols])
        pa, qa = select_rows(cells, lo, hi, OWN_CHUNKS)
        ka = select_scalar(perm, lo, hi)
        slot = cf_ref[1:2, cols].astype(jnp.float32)
        for ref, base in [(one, FACE_ROW) for one in send] + [(faces_ref, 0)]:
            ref[base + 16 * m : base + 16 * m + 8, :] = pa
            ref[base + 16 * m + 8 : base + 16 * m + 16, :] = qa
            ref[base + 128 + m : base + 129 + m, :] = ka
            ref[base + 136 + m : base + 137 + m, :] = slot
    for j in range(SLOTS):
        lo, hi = split_index(sn_ref[j : j + 1, :])
        for number, value in enumerate(select_rows(nodes, lo, hi, OWN_CHUNKS)):
            send[j][8 * number : 8 * number + 8, :] = value
        lo, hi = split_index(sc_ref[j : j + 1, :])
        pb, qb = select_rows(cells, lo, hi, OWN_CHUNKS)
        kb = jnp.broadcast_to(select_scalar(perm, lo, hi), (8, LANES))
        for ref, base in ((send[j], NODE_ROWS), (cells_ref, 24 * j)):
            ref[base : base + 8, :] = pb
            ref[base + 8 : base + 16, :] = qb
            ref[base + 16 : base + 24, :] = kb
    for copy in copies[8:]:
        copy.wait()


FACE_BLOCK = 4
ORDER = (6, 4, 2, 0, 7, 1, 5, 3)


def inner_kernel(
    d_ref, a_ref, p_ref, q_ref, k_ref, y_ref, s_ref, en_ref, if_ref, gy_ref, gp_ref, f_s, a_s, t_s, raw_s, tab_s
):
    nodes = node_tables(d_ref, a_ref)
    fill_table(raw_s, tab_s, OWN_CHUNKS, lambda number, chunk: nodes[number](chunk))
    cells = cell_tables(p_ref, q_ref)
    perm = [k_ref[0:8, :], k_ref[8:16, :]]
    width = FACE_BLOCK * LANES
    t_s[:, :width] = jnp.zeros((2, width), jnp.float32)

    def add(step, total):
        cols = pl.ds(pl.multiple_of(step * width, width), width)
        for side in range(2):
            total = total + scatter(if_ref[side : side + 1, cols], t_s[side : side + 1, cols])
        return total

    def block(step, total):
        total = add(jnp.maximum(step - 1, 0), total)
        cols = pl.ds(pl.multiple_of(step * LANES, LANES), LANES)
        elem = en_ref[:, cols]
        for pair in range(4):
            gather_pair(tab_s, elem, (2 * pair, 2 * pair + 1), 0, OWN_CHUNKS, f_s, a_s, cols)
            offset = pl.multiple_of(step * width + pair * LANES, LANES)
            ends = []
            for side in range(2):
                lo, hi = split_index(if_ref[side : side + 1, pl.ds(offset, LANES)])
                ends += select_rows(cells, lo, hi, OWN_CHUNKS) + [select_scalar(perm, lo, hi)]
            term_a, term_b = face_terms(*ends)
            t_s[0:1, pl.ds(offset, LANES)] = term_a
            t_s[1:2, pl.ds(offset, LANES)] = term_b
        return total

    steps = FI // width
    total = lax.fori_loop(0, steps, block, jnp.zeros((16, LANES), jnp.float32))
    gp_ref[...] = add(steps - 1, total)
    gy_ref[...] = -y_ref[:, :OWN] * strain_of(s_ref, f_s, a_s)


def tail_kernel(*refs):
    got = [refs[ORDER.index(j)] for j in range(SLOTS)]
    (d_ref, a_ref, cells_ref, faces_ref, y_ref, s_ref, sc_ref, en_ref, cf_ref, gyi_ref, gpi_ref) = refs[SLOTS : SLOTS + 11]
    gy_ref, gp_ref, f_s, a_s, i_s, t_s, raw_s, tab_s = refs[SLOTS + 11 :]
    own = node_tables(d_ref, a_ref)

    def read(number, chunk):
        if chunk < OWN_CHUNKS:
            return own[number](chunk)
        return got[chunk - OWN_CHUNKS][8 * number : 8 * number + 8, :]

    fill_table(raw_s, tab_s, OWN_CHUNKS + SLOTS, read)
    for step in range(EB // LANES):
        elem = en_ref[:, OWN + step * LANES : OWN + (step + 1) * LANES]
        for pair in range(4):
            gather_pair(
                tab_s,
                elem,
                (2 * pair, 2 * pair + 1),
                0,
                OWN_CHUNKS + SLOTS,
                f_s,
                a_s,
                slice(step * LANES, (step + 1) * LANES),
            )

    ghosts = [
        lambda h: got[h][NODE_ROWS : NODE_ROWS + 8, :],
        lambda h: got[h][NODE_ROWS + 8 : NODE_ROWS + 16, :],
    ]
    ghost_perm = jnp.concatenate([got[j][NODE_ROWS + 16 : NODE_ROWS + 17, :] for j in range(SLOTS)], axis=0)
    for m in range(FX // LANES):
        cols = slice(m * LANES, (m + 1) * LANES)
        lo, hi = split_index(cf_ref[1:2, cols])
        pb, qb = select_rows(ghosts, lo, hi, SLOTS)
        kb = select_scalar([ghost_perm], lo, hi)
        pa = faces_ref[16 * m : 16 * m + 8, :]
        qa = faces_ref[16 * m + 8 : 16 * m + 16, :]
        ka = faces_ref[128 + m : 129 + m, :]
        i_s[0:1, cols] = cf_ref[0:1, cols]
        t_s[0:1, cols] = face_terms(pa, qa, ka, pb, qb, kb)[0]
    for j in range(SLOTS):
        mine = j ^ 1
        pt = cells_ref[24 * mine : 24 * mine + 8, :]
        qt = cells_ref[24 * mine + 8 : 24 * mine + 16, :]
        kt = cells_ref[24 * mine + 16 : 24 * mine + 24, :]
        place = jnp.broadcast_to(sc_ref[mine : mine + 1, :], (8, LANES))
        for m in range(FX // LANES):
            cols = slice((j + 1) * FX + m * LANES, (j + 1) * FX + (m + 1) * LANES)
            lo, hi = split_index(got[j][FACE_ID + m : FACE_ID + m + 1, :].astype(jnp.int32))
            pa = got[j][FACE_ROW + 16 * m : FACE_ROW + 16 * m + 8, :]
            qa = got[j][FACE_ROW + 16 * m + 8 : FACE_ROW + 16 * m + 16, :]
            ka = got[j][FACE_K + m : FACE_K + m + 1, :]
            kb = lane_take(kt, lo)[0:1]
            term = face_terms(pa, qa, ka, lane_take(pt, lo), lane_take(qt, lo), kb)[1]
            i_s[0:1, cols] = lane_take(place, lo)[0:1]
            t_s[0:1, cols] = jnp.where(hi[0:1] == mine, term, 0.0)

    def add(step, total):
        cols = pl.ds(pl.multiple_of(step * 1024, 1024), 1024)
        return total + scatter(i_s[0:1, cols], t_s[0:1, cols])

    gp_ref[...] = lax.fori_loop(0, SLOTS + 1, add, gpi_ref[...])
    gy_ref[:, :OWN] = gyi_ref[...]
    gy_ref[:, OWN:] = -y_ref[:, OWN:] * strain_of(s_ref, f_s, a_s)


def shape(*dims):
    return jax.ShapeDtypeStruct(dims, jnp.float32)


def on_device(
    displacement,
    adjoint_disp,
    pressure,
    adjoint_pressure,
    youngs,
    permeability,
    stiffness,
    send_nodes,
    send_cells,
    elem_nodes,
    inner_faces,
    cross_faces,
):
    forward = displacement.transpose(1, 0, 2)
    adjoint = adjoint_disp.transpose(1, 0, 2)
    perm = permeability.reshape(OWN_CHUNKS, LANES)
    young = youngs.reshape(1, EL)
    sources = (
        pressure,
        adjoint_pressure,
        perm,
        cross_faces,
        send_cells,
        send_nodes,
        forward,
        adjoint,
        elem_nodes,
        inner_faces,
        young,
        stiffness,
    )
    packed = pl.pallas_call(
        pack_kernel,
        out_shape=[shape(ROWS, LANES)] * SLOTS
        + [shape(24 * SLOTS, LANES), shape(144, LANES)]
        + [jax.ShapeDtypeStruct(one.shape, one.dtype) for one in sources],
        in_specs=[pl.BlockSpec(memory_space=pltpu.HBM)] * SOURCES,
        scratch_shapes=[pltpu.SemaphoreType.DMA((SOURCES,))],
        compiler_params=VMEM,
        name="pack",
    )(*(pltpu.with_memory_space_constraint(one, pltpu.HBM) for one in sources))
    cells, faces = packed[SLOTS : SLOTS + 2]
    (
        pressure,
        adjoint_pressure,
        perm,
        cross_faces,
        send_cells,
        _,
        forward,
        adjoint,
        elem_nodes,
        inner_faces,
        young,
        stiffness,
    ) = packed[SLOTS + 2 :]
    count = lax.axis_size("dom")
    got = [
        lax.ppermute(block, "dom", [(source, (source - OFFSETS[j]) % count) for source in range(count)])
        for j, block in zip(ORDER, packed)
    ]
    inner_young, inner_perm = pl.pallas_call(
        inner_kernel,
        out_shape=[shape(1, OWN), shape(OWN_CHUNKS, LANES)],
        scratch_shapes=[
            pltpu.VMEM((192, OWN), jnp.float32),
            pltpu.VMEM((192, OWN), jnp.float32),
            pltpu.VMEM((2, FI), jnp.float32),
            pltpu.VMEM((48 * OWN_CHUNKS, LANES), jnp.float32),
            pltpu.VMEM((48 * OWN_CHUNKS, 2 * LANES), jnp.bfloat16),
        ],
        compiler_params=VMEM,
        cost_estimate=pl.CostEstimate(flops=4 * 10**9, bytes_accessed=10**7, transcendentals=0),
        name="inner",
    )(forward, adjoint, pressure, adjoint_pressure, perm, young, stiffness, elem_nodes, inner_faces)
    grad_young, grad_perm = pl.pallas_call(
        tail_kernel,
        out_shape=[shape(1, EL), shape(OWN_CHUNKS, LANES)],
        scratch_shapes=[
            pltpu.VMEM((192, EB), jnp.float32),
            pltpu.VMEM((192, EB), jnp.float32),
            pltpu.VMEM((1, (SLOTS + 1) * FX), jnp.int32),
            pltpu.VMEM((1, (SLOTS + 1) * FX), jnp.float32),
            pltpu.VMEM((48 * (OWN_CHUNKS + SLOTS), LANES), jnp.float32),
            pltpu.VMEM((48 * (OWN_CHUNKS + SLOTS), 2 * LANES), jnp.bfloat16),
        ],
        compiler_params=VMEM,
        name="tail",
    )(*got, forward, adjoint, cells, faces, young, stiffness, send_cells, elem_nodes, cross_faces, inner_young, inner_perm)
    return (grad_young.reshape(EL), grad_perm.reshape(EL))


def solution(mesh):
    in_specs = (
        P(None, None, "dom"),
        P(None, None, "dom"),
        P(None, "dom"),
        P(None, "dom"),
        P("dom"),
        P("dom"),
        P(),
        P(None, "dom"),
        P(None, "dom"),
        P(None, "dom"),
        P(None, "dom"),
        P(None, "dom"),
    )
    out_specs = (P("dom"), P("dom"))
    return jax.shard_map(
        on_device, mesh=mesh, in_specs=in_specs, out_specs=out_specs, check_vma=False
    )
```

```python
import jax
import jax.numpy as jnp
from jax import lax
from jax.experimental import pallas as pl
from jax.experimental.pallas import tpu as pltpu
from jax.sharding import PartitionSpec as P

OFFSETS = (1, -1, 2, -2, 4, -4, 8, -8)
SLOTS = 8
STEPS = 8
EL = 2048
EB = 512
OWN = EL - EB
FI = 6144
FX = 1024
LANES = 128
OWN_CHUNKS = EL // LANES
NODE_ROWS = 6 * STEPS
FACE_ROW = NODE_ROWS + 24
FACE_K = FACE_ROW + 16 * (FX // LANES)
FACE_ID = FACE_K + 8
ROWS = FACE_ID + 8
VMEM = pltpu.CompilerParams(vmem_limit_bytes=48 * 2**20)


def lane_take(table, lo):
    return jnp.take_along_axis(table, lo, axis=1, mode="promise_in_bounds")


def split_index(row):
    wide = jnp.broadcast_to(row, (8, LANES))
    return wide & (LANES - 1), wide >> 7


def select_rows(tables, lo, hi, chunks):
    picked = [lane_take(table(0), lo) for table in tables]
    for chunk in range(1, chunks):
        here = hi == chunk
        picked = [jnp.where(here, lane_take(table(chunk), lo), old) for table, old in zip(tables, picked)]
    return picked


def select_scalar(blocks, lo, hi):
    sub = lax.broadcasted_iota(jnp.int32, (8, LANES), 0)
    total = None
    for number, block in enumerate(blocks):
        part = jnp.where(hi == sub + 8 * number, lane_take(block, lo), 0.0)
        total = part if total is None else total + part
    return jnp.sum(total, axis=0, keepdims=True)


def cell_tables(p_ref, q_ref):
    return [
        lambda h: p_ref[:, h * LANES : (h + 1) * LANES],
        lambda h: q_ref[:, h * LANES : (h + 1) * LANES],
    ]


def node_tables(d_ref, a_ref):
    def table(ref, comp):
        return lambda h: ref[comp, :, h * LANES : (h + 1) * LANES]

    return [table(d_ref, comp) for comp in range(3)] + [table(a_ref, comp) for comp in range(3)]


def face_terms(pa, qa, ka, pb, qb, kb):
    product = jnp.sum((pa - pb) * (qa - qb), axis=0, keepdims=True)
    total = ka + kb
    common = 2.0 * ka * kb * product / (total * total)
    return common * kb, common * ka


def scatter(index, term):
    length = index.shape[1]
    lo = index & (LANES - 1)
    hi = index >> 7
    hot = jnp.where(lax.broadcasted_iota(jnp.int32, (LANES, length), 0) == lo, 1.0, 0.0).astype(jnp.bfloat16)
    top = term.astype(jnp.bfloat16).astype(jnp.float32)
    rows = lax.broadcasted_iota(jnp.int32, (16, length), 0) == hi
    left = jnp.concatenate([jnp.where(rows, top, 0.0), jnp.where(rows, term - top, 0.0)], axis=0)
    out = lax.dot_general(
        left.astype(jnp.bfloat16), hot, (((1,), (1,)), ((), ())), preferred_element_type=jnp.float32
    )
    return out[:16] + out[16:]


def halves(value):
    top = value.astype(jnp.bfloat16)
    return top, (value - top.astype(jnp.float32)).astype(jnp.bfloat16)


def spread_stiffness(k_ref):
    pick = (
        lax.broadcasted_iota(jnp.int32, (192, 24), 0) // 8 == lax.broadcasted_iota(jnp.int32, (192, 24), 1)
    ).astype(jnp.float32).astype(jnp.bfloat16)
    same = (lax.broadcasted_iota(jnp.int32, (192, 192), 0) & 7) == (
        lax.broadcasted_iota(jnp.int32, (192, 192), 1) & 7
    )
    out = []
    for half in halves(k_ref[...]):
        tall = jnp.dot(pick, half, preferred_element_type=jnp.float32).astype(jnp.bfloat16)
        full = lax.dot_general(tall, pick, (((1,), (1,)), ((), ())), preferred_element_type=jnp.float32)
        out.append(jnp.where(same, full, 0.0).astype(jnp.bfloat16))
    return out


def strain_of(k_ref, f_ref, a_ref):
    top, low = spread_stiffness(k_ref)
    f_top, f_low = halves(f_ref[...])
    weighted = jnp.dot(top, f_top, preferred_element_type=jnp.float32)
    weighted += jnp.dot(low, f_top, preferred_element_type=jnp.float32)
    weighted += jnp.dot(top, f_low, preferred_element_type=jnp.float32)
    return jnp.sum(a_ref[...] * weighted, axis=0, keepdims=True)


def fill_table(raw_ref, tab_ref, chunks, read):
    for chunk in range(chunks):
        for number in range(6):
            line = 48 * chunk + 8 * number
            raw_ref[line : line + 8, :] = read(number, chunk)
    top, low = halves(raw_ref[...])
    tab_ref[:, :LANES] = top
    tab_ref[:, LANES:] = low


def gather_pair(tab_ref, elem, corners, first, last, f_ref, a_ref, cols, old_f=None, old_a=None):
    sub = lax.broadcasted_iota(jnp.int32, (LANES, LANES), 0)
    hot = jnp.concatenate(
        [jnp.where(sub == (elem[n : n + 1] & (LANES - 1)), 1.0, 0.0).astype(jnp.bfloat16) for n in corners], axis=1
    )
    found = jnp.dot(tab_ref[...], jnp.concatenate([hot, hot], axis=0), preferred_element_type=jnp.float32)
    for place, corner in enumerate(corners):
        hi = jnp.broadcast_to(elem[corner : corner + 1] >> 7, (8, LANES))
        lines = [(8 * comp + corner) * 8 for comp in range(3)]
        if old_f is None or corner == 0:
            got = [None] * 6
        else:
            got = [ref[line : line + 8, cols] for ref in (old_f, old_a) for line in lines]
        for chunk in range(first, last):
            base = 48 * (chunk - first)
            new = [found[base + 8 * r : base + 8 * r + 8, place * LANES : (place + 1) * LANES] for r in range(6)]
            here = hi == chunk
            got = [fresh if old is None else jnp.where(here, fresh, old) for fresh, old in zip(new, got)]
        for comp, line in enumerate(lines):
            f_ref[line : line + 8, cols] = got[comp]
            a_ref[line : line + 8, cols] = got[3 + comp]


SOURCES = 12


def pack_kernel(*refs):
    sources, outs, sem = refs[:SOURCES], refs[SOURCES:-1], refs[-1]
    far_ref, near_refs, cells_ref, faces_ref = outs[0], outs[1 : NEAR + 1], outs[NEAR + 1], outs[NEAR + 2]
    local = outs[NEAR + 3 :]
    copies = [pltpu.make_async_copy(far, near, sem.at[n]) for n, (far, near) in enumerate(zip(sources, local))]
    for copy in copies:
        copy.start()
    for copy in copies[:8]:
        copy.wait()
    p_ref, q_ref, k_ref, cf_ref, sc_ref, sn_ref, d_ref, a_ref = local[:8]
    nodes = node_tables(d_ref, a_ref)
    cells = cell_tables(p_ref, q_ref)
    perm = [k_ref[0:8, :], k_ref[8:16, :]]
    for m in range(FX // LANES):
        cols = slice(m * LANES, (m + 1) * LANES)
        lo, hi = split_index(cf_ref[0:1, cols])
        pa, qa = select_rows(cells, lo, hi, OWN_CHUNKS)
        ka = select_scalar(perm, lo, hi)
        slot = cf_ref[1:2, cols].astype(jnp.float32)
        for ref, base in [(one, FACE_ROW) for one in near_refs] + [(faces_ref, 0), (far_ref, FAR_FACES)]:
            ref[base + 16 * m : base + 16 * m + 8, :] = pa
            ref[base + 16 * m + 8 : base + 16 * m + 16, :] = qa
            ref[base + 128 + m : base + 129 + m, :] = ka
            ref[base + 136 + m : base + 137 + m, :] = slot
    for j in (6, 7) + ORDER:
        out, start = (near_refs[ORDER.index(j)], 0) if j < NEAR else (far_ref, BLOCK * (j - NEAR))
        lo, hi = split_index(sn_ref[j : j + 1, :])
        for number, value in enumerate(select_rows(nodes, lo, hi, OWN_CHUNKS)):
            out[start + 8 * number : start + 8 * number + 8, :] = value
        lo, hi = split_index(sc_ref[j : j + 1, :])
        pb, qb = select_rows(cells, lo, hi, OWN_CHUNKS)
        kb = jnp.broadcast_to(select_scalar(perm, lo, hi), (8, LANES))
        for ref, base in ((out, start + NODE_ROWS), (cells_ref, 24 * j)):
            ref[base : base + 8, :] = pb
            ref[base + 8 : base + 16, :] = qb
            ref[base + 16 : base + 24, :] = kb
    for copy in copies[8:]:
        copy.wait()


FACE_BLOCK = 4
ORDER = (2, 4, 0, 1, 5, 3)
NEAR = len(ORDER)
BLOCK = NODE_ROWS + 24
FAR_FACES = 2 * BLOCK
FAR_ROWS = FAR_FACES + 144


def inner_kernel(
    d_ref, a_ref, p_ref, q_ref, k_ref, y_ref, s_ref, en_ref, if_ref, gy_ref, gp_ref, tab_s, f_s, a_s, t_s, raw_s
):
    nodes = node_tables(d_ref, a_ref)
    fill_table(raw_s, tab_s, OWN_CHUNKS, lambda number, chunk: nodes[number](chunk))
    cells = cell_tables(p_ref, q_ref)
    perm = [k_ref[0:8, :], k_ref[8:16, :]]
    width = FACE_BLOCK * LANES
    t_s[:, :width] = jnp.zeros((2, width), jnp.float32)

    def add(step, total):
        cols = pl.ds(pl.multiple_of(step * width, width), width)
        for side in range(2):
            total = total + scatter(if_ref[side : side + 1, cols], t_s[side : side + 1, cols])
        return total

    def block(step, total):
        total = add(jnp.maximum(step - 1, 0), total)
        cols = pl.ds(pl.multiple_of(step * LANES, LANES), LANES)
        elem = en_ref[:, cols]
        for pair in range(4):
            gather_pair(tab_s, elem, (2 * pair, 2 * pair + 1), 0, OWN_CHUNKS, f_s, a_s, cols)
            offset = pl.multiple_of(step * width + pair * LANES, LANES)
            ends = []
            for side in range(2):
                lo, hi = split_index(if_ref[side : side + 1, pl.ds(offset, LANES)])
                ends += select_rows(cells, lo, hi, OWN_CHUNKS) + [select_scalar(perm, lo, hi)]
            term_a, term_b = face_terms(*ends)
            t_s[0:1, pl.ds(offset, LANES)] = term_a
            t_s[1:2, pl.ds(offset, LANES)] = term_b
        return total

    steps = FI // width
    total = lax.fori_loop(0, steps, block, jnp.zeros((16, LANES), jnp.float32))
    gp_ref[...] = add(steps - 1, total)
    gy_ref[...] = -y_ref[:, :OWN] * strain_of(s_ref, f_s, a_s)


def edge_kernel(tab_ref, en_ref, f_ref, a_ref):
    def block(step, _):
        start = pl.multiple_of(step * LANES, LANES)
        elem = en_ref[:, pl.ds(pl.multiple_of(OWN + start, LANES), LANES)]
        for pair in range(4):
            gather_pair(tab_ref, elem, (2 * pair, 2 * pair + 1), 0, OWN_CHUNKS, f_ref, a_ref, pl.ds(start, LANES))
        return 0

    lax.fori_loop(0, EB // LANES, block, 0)


def tail_kernel(*refs):
    near, (swapped, relayed) = refs[:NEAR], refs[NEAR : NEAR + 2]
    (fo_ref, ao_ref, cells_ref, faces_ref, y_ref, s_ref, sc_ref, en_ref, cf_ref, gyi_ref, gpi_ref) = refs[NEAR + 2 : NEAR + 13]
    gy_ref, gp_ref, f_s, a_s, i_s, t_s, raw_s, tab_s, up_s, down_s = refs[NEAR + 13 :]
    got = [near[ORDER.index(j)] for j in range(NEAR)] + [up_s, down_s]
    low = jnp.broadcast_to((lax.axis_index("dom") & 8) == 0, (8, LANES))
    for ref, start, direct, other in ((up_s, 0, swapped, relayed), (down_s, BLOCK, relayed, swapped)):
        for to, source, length in ((0, start, BLOCK), (BLOCK, FAR_FACES, 144)):
            for row in range(0, length, 8):
                ref[to + row : to + row + 8, :] = jnp.where(
                    low, direct[source + row : source + row + 8, :], other[source + row : source + row + 8, :]
                )
    fill_table(raw_s, tab_s, SLOTS, lambda number, chunk: got[chunk][8 * number : 8 * number + 8, :])
    for step in range(EB // LANES):
        elem = en_ref[:, OWN + step * LANES : OWN + (step + 1) * LANES]
        cols = slice(step * LANES, (step + 1) * LANES)
        for pair in range(4):
            corners = (2 * pair, 2 * pair + 1)
            gather_pair(tab_s, elem, corners, OWN_CHUNKS, OWN_CHUNKS + SLOTS, f_s, a_s, cols, fo_ref, ao_ref)

    ghosts = [
        lambda h: got[h][NODE_ROWS : NODE_ROWS + 8, :],
        lambda h: got[h][NODE_ROWS + 8 : NODE_ROWS + 16, :],
    ]
    ghost_perm = jnp.concatenate([got[j][NODE_ROWS + 16 : NODE_ROWS + 17, :] for j in range(SLOTS)], axis=0)
    for m in range(FX // LANES):
        cols = slice(m * LANES, (m + 1) * LANES)
        lo, hi = split_index(cf_ref[1:2, cols])
        pb, qb = select_rows(ghosts, lo, hi, SLOTS)
        kb = select_scalar([ghost_perm], lo, hi)
        pa = faces_ref[16 * m : 16 * m + 8, :]
        qa = faces_ref[16 * m + 8 : 16 * m + 16, :]
        ka = faces_ref[128 + m : 129 + m, :]
        i_s[0:1, cols] = cf_ref[0:1, cols]
        t_s[0:1, cols] = face_terms(pa, qa, ka, pb, qb, kb)[0]
    for j in range(SLOTS):
        mine = j ^ 1
        pt = cells_ref[24 * mine : 24 * mine + 8, :]
        qt = cells_ref[24 * mine + 8 : 24 * mine + 16, :]
        kt = cells_ref[24 * mine + 16 : 24 * mine + 24, :]
        place = jnp.broadcast_to(sc_ref[mine : mine + 1, :], (8, LANES))
        for m in range(FX // LANES):
            cols = slice((j + 1) * FX + m * LANES, (j + 1) * FX + (m + 1) * LANES)
            lo, hi = split_index(got[j][FACE_ID + m : FACE_ID + m + 1, :].astype(jnp.int32))
            pa = got[j][FACE_ROW + 16 * m : FACE_ROW + 16 * m + 8, :]
            qa = got[j][FACE_ROW + 16 * m + 8 : FACE_ROW + 16 * m + 16, :]
            ka = got[j][FACE_K + m : FACE_K + m + 1, :]
            kb = lane_take(kt, lo)[0:1]
            term = face_terms(pa, qa, ka, lane_take(pt, lo), lane_take(qt, lo), kb)[1]
            i_s[0:1, cols] = lane_take(place, lo)[0:1]
            t_s[0:1, cols] = jnp.where(hi[0:1] == mine, term, 0.0)

    def add(step, total):
        cols = pl.ds(pl.multiple_of(step * 1024, 1024), 1024)
        return total + scatter(i_s[0:1, cols], t_s[0:1, cols])

    gp_ref[...] = lax.fori_loop(0, SLOTS + 1, add, gpi_ref[...])
    gy_ref[:, :OWN] = gyi_ref[...]
    gy_ref[:, OWN:] = -y_ref[:, OWN:] * strain_of(s_ref, f_s, a_s)


def shape(*dims):
    return jax.ShapeDtypeStruct(dims, jnp.float32)


def on_device(
    displacement,
    adjoint_disp,
    pressure,
    adjoint_pressure,
    youngs,
    permeability,
    stiffness,
    send_nodes,
    send_cells,
    elem_nodes,
    inner_faces,
    cross_faces,
):
    forward = displacement.transpose(1, 0, 2)
    adjoint = adjoint_disp.transpose(1, 0, 2)
    perm = permeability.reshape(OWN_CHUNKS, LANES)
    young = youngs.reshape(1, EL)
    sources = (
        pressure,
        adjoint_pressure,
        perm,
        cross_faces,
        send_cells,
        send_nodes,
        forward,
        adjoint,
        elem_nodes,
        inner_faces,
        young,
        stiffness,
    )
    packed = pl.pallas_call(
        pack_kernel,
        out_shape=[shape(FAR_ROWS, LANES)]
        + [shape(ROWS, LANES)] * NEAR
        + [shape(24 * SLOTS, LANES), shape(144, LANES)]
        + [jax.ShapeDtypeStruct(one.shape, one.dtype) for one in sources],
        in_specs=[pl.BlockSpec(memory_space=pltpu.HBM)] * SOURCES,
        scratch_shapes=[pltpu.SemaphoreType.DMA((SOURCES,))],
        compiler_params=VMEM,
        name="pack",
    )(*(pltpu.with_memory_space_constraint(one, pltpu.HBM) for one in sources))
    cells, faces = packed[NEAR + 1 : NEAR + 3]
    (
        pressure,
        adjoint_pressure,
        perm,
        cross_faces,
        send_cells,
        _,
        forward,
        adjoint,
        elem_nodes,
        inner_faces,
        young,
        stiffness,
    ) = packed[NEAR + 3 :]
    count = lax.axis_size("dom")
    swapped = lax.ppermute(packed[0], "dom", [(source, source ^ 8) for source in range(count)])
    near = [
        lax.ppermute(block, "dom", [(source, (source - OFFSETS[j]) % count) for source in range(count)])
        for j, block in zip(ORDER, packed[1:])
    ]
    inner_young, inner_perm, table = pl.pallas_call(
        inner_kernel,
        out_shape=[
            shape(1, OWN),
            shape(OWN_CHUNKS, LANES),
            jax.ShapeDtypeStruct((48 * OWN_CHUNKS, 2 * LANES), jnp.bfloat16),
        ],
        scratch_shapes=[
            pltpu.VMEM((192, OWN), jnp.float32),
            pltpu.VMEM((192, OWN), jnp.float32),
            pltpu.VMEM((2, FI), jnp.float32),
            pltpu.VMEM((48 * OWN_CHUNKS, LANES), jnp.float32),
        ],
        compiler_params=VMEM,
        cost_estimate=pl.CostEstimate(flops=4 * 10**9, bytes_accessed=10**7, transcendentals=0),
        name="inner",
    )(forward, adjoint, pressure, adjoint_pressure, perm, young, stiffness, elem_nodes, inner_faces)
    swapped, inner_young, inner_perm, table = lax.optimization_barrier((swapped, inner_young, inner_perm, table))
    relayed = lax.ppermute(
        swapped, "dom", [(source, (source - 16 if source & 8 else source + 16) % count) for source in range(count)]
    )
    edge_forward, edge_adjoint = pl.pallas_call(
        edge_kernel,
        out_shape=[shape(192, EB), shape(192, EB)],
        compiler_params=VMEM,
        cost_estimate=pl.CostEstimate(flops=2 * 10**9, bytes_accessed=10**7, transcendentals=0),
        name="edge",
    )(table, elem_nodes)
    grad_young, grad_perm = pl.pallas_call(
        tail_kernel,
        out_shape=[shape(1, EL), shape(OWN_CHUNKS, LANES)],
        scratch_shapes=[
            pltpu.VMEM((192, EB), jnp.float32),
            pltpu.VMEM((192, EB), jnp.float32),
            pltpu.VMEM((1, (SLOTS + 1) * FX), jnp.int32),
            pltpu.VMEM((1, (SLOTS + 1) * FX), jnp.float32),
            pltpu.VMEM((48 * SLOTS, LANES), jnp.float32),
            pltpu.VMEM((48 * SLOTS, 2 * LANES), jnp.bfloat16),
            pltpu.VMEM((ROWS, LANES), jnp.float32),
            pltpu.VMEM((ROWS, LANES), jnp.float32),
        ],
        compiler_params=VMEM,
        name="tail",
    )(*near, swapped, relayed, edge_forward, edge_adjoint, cells, faces, young, stiffness, send_cells, elem_nodes, cross_faces, inner_young, inner_perm)
    return (grad_young.reshape(EL), grad_perm.reshape(EL))


def solution(mesh):
    in_specs = (
        P(None, None, "dom"),
        P(None, None, "dom"),
        P(None, "dom"),
        P(None, "dom"),
        P("dom"),
        P("dom"),
        P(),
        P(None, "dom"),
        P(None, "dom"),
        P(None, "dom"),
        P(None, "dom"),
        P(None, "dom"),
    )
    out_specs = (P("dom"), P("dom"))
    return jax.shard_map(
        on_device, mesh=mesh, in_specs=in_specs, out_specs=out_specs, check_vma=False
    )
```

```python
import jax
import jax.numpy as jnp
from jax import lax
from jax.experimental import pallas as pl
from jax.experimental.pallas import tpu as pltpu
from jax.sharding import PartitionSpec as P


OFFSETS = (1, -1, 2, -2, 4, -4, 8, -8)
SLOTS = 8
STEPS = 8
EL = 2048
EB = 512
OWN = EL - EB
FI = 6144
FX = 1024
LANES = 128
OWN_CHUNKS = EL // LANES
NODE_ROWS = 6 * STEPS
FACE_ROW = NODE_ROWS + 24
FACE_K = FACE_ROW + 16 * (FX // LANES)
FACE_ID = FACE_K + 8
ROWS = FACE_ID + 8
VMEM = pltpu.CompilerParams(vmem_limit_bytes=48 * 2**20)


def lane_take(table, lo):
    return jnp.take_along_axis(table, lo, axis=1, mode="promise_in_bounds")


def split_index(row):
    wide = jnp.broadcast_to(row, (8, LANES))
    return wide & (LANES - 1), wide >> 7


def select_rows(tables, lo, hi, chunks):
    picked = [lane_take(table(0), lo) for table in tables]
    for chunk in range(1, chunks):
        here = hi == chunk
        picked = [jnp.where(here, lane_take(table(chunk), lo), old) for table, old in zip(tables, picked)]
    return picked


def select_scalar(blocks, lo, hi):
    sub = lax.broadcasted_iota(jnp.int32, (8, LANES), 0)
    total = None
    for number, block in enumerate(blocks):
        part = jnp.where(hi == sub + 8 * number, lane_take(block, lo), 0.0)
        total = part if total is None else total + part
    return jnp.sum(total, axis=0, keepdims=True)


def cell_tables(p_ref, q_ref):
    return [
        lambda h: p_ref[:, h * LANES : (h + 1) * LANES],
        lambda h: q_ref[:, h * LANES : (h + 1) * LANES],
    ]


def node_tables(d_ref, a_ref):
    def table(ref, comp):
        return lambda h: ref[comp, :, h * LANES : (h + 1) * LANES]

    return [table(d_ref, comp) for comp in range(3)] + [table(a_ref, comp) for comp in range(3)]


def face_terms(pa, qa, ka, pb, qb, kb):
    product = jnp.sum((pa - pb) * (qa - qb), axis=0, keepdims=True)
    total = ka + kb
    common = 2.0 * ka * kb * product / (total * total)
    return common * kb, common * ka


def scatter(index, term):
    length = index.shape[1]
    lo = index & (LANES - 1)
    hi = index >> 7
    hot = jnp.where(lax.broadcasted_iota(jnp.int32, (LANES, length), 0) == lo, 1.0, 0.0).astype(jnp.bfloat16)
    top = term.astype(jnp.bfloat16).astype(jnp.float32)
    rows = lax.broadcasted_iota(jnp.int32, (16, length), 0) == hi
    left = jnp.concatenate([jnp.where(rows, top, 0.0), jnp.where(rows, term - top, 0.0)], axis=0)
    out = lax.dot_general(
        left.astype(jnp.bfloat16), hot, (((1,), (1,)), ((), ())), preferred_element_type=jnp.float32
    )
    return out[:16] + out[16:]


def halves(value):
    top = value.astype(jnp.bfloat16)
    return top, (value - top.astype(jnp.float32)).astype(jnp.bfloat16)


def spread_stiffness(k_ref):
    pick = (
        lax.broadcasted_iota(jnp.int32, (192, 24), 0) // 8 == lax.broadcasted_iota(jnp.int32, (192, 24), 1)
    ).astype(jnp.float32).astype(jnp.bfloat16)
    same = (lax.broadcasted_iota(jnp.int32, (192, 192), 0) & 7) == (
        lax.broadcasted_iota(jnp.int32, (192, 192), 1) & 7
    )
    out = []
    for half in halves(k_ref[...]):
        tall = jnp.dot(pick, half, preferred_element_type=jnp.float32).astype(jnp.bfloat16)
        full = lax.dot_general(tall, pick, (((1,), (1,)), ((), ())), preferred_element_type=jnp.float32)
        out.append(jnp.where(same, full, 0.0).astype(jnp.bfloat16))
    return out


def strain_of(k_ref, f_ref, a_ref):
    top, low = spread_stiffness(k_ref)
    f_top, f_low = halves(f_ref[...])
    weighted = jnp.dot(top, f_top, preferred_element_type=jnp.float32)
    weighted += jnp.dot(low, f_top, preferred_element_type=jnp.float32)
    weighted += jnp.dot(top, f_low, preferred_element_type=jnp.float32)
    return jnp.sum(a_ref[...] * weighted, axis=0, keepdims=True)


def fill_table(raw_ref, tab_ref, chunks, read):
    for chunk in range(chunks):
        for number in range(6):
            line = 48 * chunk + 8 * number
            raw_ref[line : line + 8, :] = read(number, chunk)
    top, low = halves(raw_ref[...])
    tab_ref[:, :LANES] = top
    tab_ref[:, LANES:] = low


def lookup(tab_ref, rows, first, last, olds=(None, None)):
    sub = lax.broadcasted_iota(jnp.int32, (LANES, LANES), 0)
    hot = jnp.concatenate(
        [jnp.where(sub == (row & (LANES - 1)), 1.0, 0.0).astype(jnp.bfloat16) for row in rows], axis=1
    )
    found = jnp.dot(tab_ref[...], jnp.concatenate([hot, hot], axis=0), preferred_element_type=jnp.float32)
    results = []
    for place, (row, old) in enumerate(zip(rows, olds)):
        hi = jnp.broadcast_to(row >> 7, (8, LANES))
        got = [None] * 6 if old is None else old
        for chunk in range(first, last):
            base = 48 * (chunk - first)
            new = [found[base + 8 * r : base + 8 * r + 8, place * LANES : (place + 1) * LANES] for r in range(6)]
            here = hi == chunk
            got = [fresh if kept is None else jnp.where(here, fresh, kept) for fresh, kept in zip(new, got)]
        results.append(got)
    return results


def lines(corner):
    return [(8 * comp + corner) * 8 for comp in range(3)]


def put(f_ref, a_ref, corner, cols, got):
    for comp, line in enumerate(lines(corner)):
        f_ref[line : line + 8, cols] = got[comp]
        a_ref[line : line + 8, cols] = got[3 + comp]


def own_corners(tab_ref, nodes, elem, pairs, lone, f_ref, a_ref, cols):
    for pair in pairs:
        for corner, got in zip(pair, lookup(tab_ref, [elem[n : n + 1] for n in pair], 0, OWN_CHUNKS)):
            put(f_ref, a_ref, corner, cols, got)
    for corner in lone:
        lo, hi = split_index(elem[corner : corner + 1])
        put(f_ref, a_ref, corner, cols, select_rows(nodes, lo, hi, OWN_CHUNKS))


def ghost_corners(tab_ref, elem, first, last, old_f, old_a, f_ref, a_ref, cols, fresh):
    for pair in range(4):
        corners = (2 * pair, 2 * pair + 1)
        olds = [
            None
            if corner == 0 and fresh
            else [ref[line : line + 8, cols] for ref in (old_f, old_a) for line in lines(corner)]
            for corner in corners
        ]
        for corner, got in zip(corners, lookup(tab_ref, [elem[n : n + 1] for n in corners], first, last, olds)):
            put(f_ref, a_ref, corner, cols, got)


SOURCES = 12


def pack_kernel(*refs):
    sources, outs, raw_s, sem = refs[:SOURCES], refs[SOURCES:-2], refs[-2], refs[-1]
    far_ref, near_refs, cells_ref, faces_ref = outs[0], outs[1 : NEAR + 1], outs[NEAR + 1], outs[NEAR + 2]
    tab_ref, local = outs[NEAR + 3], outs[NEAR + 4 :]
    copies = [pltpu.make_async_copy(far, near, sem.at[n]) for n, (far, near) in enumerate(zip(sources, local))]
    for copy in copies:
        copy.start()
    for copy in copies[:8]:
        copy.wait()
    p_ref, q_ref, k_ref, cf_ref, sc_ref, sn_ref, d_ref, a_ref = local[:8]
    nodes = node_tables(d_ref, a_ref)
    cells = cell_tables(p_ref, q_ref)
    perm = [k_ref[0:8, :], k_ref[8:16, :]]
    for m in range(FX // LANES):
        cols = slice(m * LANES, (m + 1) * LANES)
        lo, hi = split_index(cf_ref[0:1, cols])
        pa, qa = select_rows(cells, lo, hi, OWN_CHUNKS)
        ka = select_scalar(perm, lo, hi)
        slot = cf_ref[1:2, cols].astype(jnp.float32)
        for ref, base in [(one, FACE_ROW) for one in near_refs] + [(faces_ref, 0), (far_ref, FAR_FACES)]:
            ref[base + 16 * m : base + 16 * m + 8, :] = pa
            ref[base + 16 * m + 8 : base + 16 * m + 16, :] = qa
            ref[base + 128 + m : base + 129 + m, :] = ka
            ref[base + 136 + m : base + 137 + m, :] = slot
    fill_table(raw_s, tab_ref, OWN_CHUNKS, lambda number, chunk: nodes[number](chunk))
    for j in range(SLOTS):
        out, start = (near_refs[ORDER.index(j)], 0) if j < NEAR else (far_ref, BLOCK * (j - NEAR))
        if j % 2 == 0:
            both = lookup(tab_ref, [sn_ref[n : n + 1, :] for n in (j, j + 1)], 0, OWN_CHUNKS)
        for number, value in enumerate(both[j % 2]):
            out[start + 8 * number : start + 8 * number + 8, :] = value
        lo, hi = split_index(sc_ref[j : j + 1, :])
        pb, qb = select_rows(cells, lo, hi, OWN_CHUNKS)
        kb = jnp.broadcast_to(select_scalar(perm, lo, hi), (8, LANES))
        for ref, base in ((out, start + NODE_ROWS), (cells_ref, 24 * j)):
            ref[base : base + 8, :] = pb
            ref[base + 8 : base + 16, :] = qb
            ref[base + 16 : base + 24, :] = kb
    for copy in copies[8:]:
        copy.wait()


FACE_BLOCK = 6
EARLY = FI // FACE_BLOCK
ORDER = (2, 4, 0, 1, 5, 3)
NEAR = len(ORDER)
BLOCK = NODE_ROWS + 24
FAR_FACES = 2 * BLOCK
FAR_ROWS = FAR_FACES + 144


def inner_kernel(tab_ref, p_ref, q_ref, k_ref, y_ref, s_ref, en_ref, if_ref, gy_ref, gp_ref, f_s, a_s, t_s):
    cells = cell_tables(p_ref, q_ref)
    perm = [k_ref[0:8, :], k_ref[8:16, :]]
    width = FACE_BLOCK * LANES
    t_s[:, :width] = jnp.zeros((2, width), jnp.float32)

    def add(step, total):
        cols = pl.ds(pl.multiple_of(step * width, width), width)
        for side in range(2):
            total = total + scatter(if_ref[side : side + 1, cols], t_s[side : side + 1, cols])
        return total

    def block(step, total):
        total = add(jnp.maximum(step - 1, 0), total)
        cols = pl.ds(pl.multiple_of(step * LANES, LANES), LANES)
        elem = en_ref[:, cols]
        own_corners(tab_ref, None, elem, ((0, 1), (2, 3), (4, 5), (6, 7)), (), f_s, a_s, cols)
        for face in range(FACE_BLOCK):
            offset = pl.multiple_of(step * width + face * LANES, LANES)
            ends = []
            for side in range(2):
                lo, hi = split_index(if_ref[side : side + 1, pl.ds(offset, LANES)])
                ends += select_rows(cells, lo, hi, OWN_CHUNKS) + [select_scalar(perm, lo, hi)]
            term_a, term_b = face_terms(*ends)
            t_s[0:1, pl.ds(offset, LANES)] = term_a
            t_s[1:2, pl.ds(offset, LANES)] = term_b
        return total

    steps = FI // width
    total = lax.fori_loop(0, steps, block, jnp.zeros((16, LANES), jnp.float32))
    gp_ref[...] = add(steps - 1, total)
    gy_ref[...] = -y_ref[:, :EARLY] * strain_of(s_ref, f_s, a_s)


def edge_kernel(tab_ref, d_ref, a_ref, y_ref, s_ref, en_ref, gyi_ref, gy_ref, fo_ref, ao_ref, f_s, a_s):
    nodes = node_tables(d_ref, a_ref)

    def block(step, _):
        start = pl.multiple_of(step * LANES, LANES)
        cols = pl.ds(start, LANES)
        elem = en_ref[:, pl.ds(pl.multiple_of(EARLY + start, LANES), LANES)]
        own_corners(tab_ref, nodes, elem, ((0, 1), (2, 3), (4, 5)), (6, 7), f_s, a_s, cols)
        elem = en_ref[:, pl.ds(pl.multiple_of(OWN + start, LANES), LANES)]
        own_corners(tab_ref, nodes, elem, ((1, 2), (3, 4)), (5, 6, 7), fo_ref, ao_ref, cols)
        return 0

    lax.fori_loop(0, EB // LANES, block, 0)
    gy_ref[:, :EARLY] = gyi_ref[...]
    gy_ref[:, EARLY:] = -y_ref[:, EARLY:OWN] * strain_of(s_ref, f_s, a_s)


def incoming(got, cells_ref, sc_ref, slots, i_s, t_s, start):
    for number, j in enumerate(slots):
        mine = j ^ 1
        pt = cells_ref[24 * mine : 24 * mine + 8, :]
        qt = cells_ref[24 * mine + 8 : 24 * mine + 16, :]
        kt = cells_ref[24 * mine + 16 : 24 * mine + 24, :]
        place = jnp.broadcast_to(sc_ref[mine : mine + 1, :], (8, LANES))
        for m in range(FX // LANES):
            base = start + number * FX + m * LANES
            cols = slice(base, base + LANES)
            lo, hi = split_index(got[j][FACE_ID + m : FACE_ID + m + 1, :].astype(jnp.int32))
            pa = got[j][FACE_ROW + 16 * m : FACE_ROW + 16 * m + 8, :]
            qa = got[j][FACE_ROW + 16 * m + 8 : FACE_ROW + 16 * m + 16, :]
            ka = got[j][FACE_K + m : FACE_K + m + 1, :]
            kb = lane_take(kt, lo)[0:1]
            term = face_terms(pa, qa, ka, lane_take(pt, lo), lane_take(qt, lo), kb)[1]
            i_s[0:1, cols] = lane_take(place, lo)[0:1]
            t_s[0:1, cols] = jnp.where(hi[0:1] == mine, term, 0.0)


def add_terms(i_s, t_s, count, total):
    def add(step, total):
        cols = pl.ds(pl.multiple_of(step * 1024, 1024), 1024)
        return total + scatter(i_s[0:1, cols], t_s[0:1, cols])

    return lax.fori_loop(0, count, add, total)


def near_kernel(*refs):
    near, (fo_ref, ao_ref, cells_ref, sc_ref, en_ref, gpi_ref) = refs[:NEAR], refs[NEAR : NEAR + 6]
    f_ref, a_ref, gp_ref, i_s, t_s, raw_s, tab_s = refs[NEAR + 6 :]
    got = [near[ORDER.index(j)] for j in range(NEAR)]
    fill_table(raw_s, tab_s, NEAR, lambda number, chunk: got[chunk][8 * number : 8 * number + 8, :])
    for step in range(EB // LANES):
        elem = en_ref[:, OWN + step * LANES : OWN + (step + 1) * LANES]
        cols = slice(step * LANES, (step + 1) * LANES)
        ghost_corners(tab_s, elem, OWN_CHUNKS, OWN_CHUNKS + NEAR, fo_ref, ao_ref, f_ref, a_ref, cols, True)
    incoming(got, cells_ref, sc_ref, range(NEAR), i_s, t_s, 0)
    gp_ref[...] = add_terms(i_s, t_s, NEAR, gpi_ref[...])


def tail_kernel(*refs):
    near, (swapped, relayed) = refs[:NEAR], refs[NEAR : NEAR + 2]
    (fo_ref, ao_ref, cells_ref, faces_ref, y_ref, s_ref, sc_ref, en_ref, cf_ref, gyi_ref, gpi_ref) = refs[NEAR + 2 : NEAR + 13]
    gy_ref, gp_ref, f_s, a_s, i_s, t_s, raw_s, tab_s, up_s, down_s = refs[NEAR + 13 :]
    got = [near[ORDER.index(j)] for j in range(NEAR)] + [up_s, down_s]
    low = jnp.broadcast_to((lax.axis_index("dom") & 8) == 0, (8, LANES))
    for ref, start, direct, other in ((up_s, 0, swapped, relayed), (down_s, BLOCK, relayed, swapped)):
        for to, source, length in ((0, start, BLOCK), (BLOCK, FAR_FACES, 144)):
            for row in range(0, length, 8):
                ref[to + row : to + row + 8, :] = jnp.where(
                    low, direct[source + row : source + row + 8, :], other[source + row : source + row + 8, :]
                )
    fill_table(raw_s, tab_s, 2, lambda number, chunk: got[NEAR + chunk][8 * number : 8 * number + 8, :])
    for step in range(EB // LANES):
        elem = en_ref[:, OWN + step * LANES : OWN + (step + 1) * LANES]
        cols = slice(step * LANES, (step + 1) * LANES)
        ghost_corners(
            tab_s, elem, OWN_CHUNKS + NEAR, OWN_CHUNKS + SLOTS, fo_ref, ao_ref, f_s, a_s, cols, False
        )

    ghosts = [
        lambda h: got[h][NODE_ROWS : NODE_ROWS + 8, :],
        lambda h: got[h][NODE_ROWS + 8 : NODE_ROWS + 16, :],
    ]
    ghost_perm = jnp.concatenate([got[j][NODE_ROWS + 16 : NODE_ROWS + 17, :] for j in range(SLOTS)], axis=0)
    for m in range(FX // LANES):
        cols = slice(m * LANES, (m + 1) * LANES)
        lo, hi = split_index(cf_ref[1:2, cols])
        pb, qb = select_rows(ghosts, lo, hi, SLOTS)
        kb = select_scalar([ghost_perm], lo, hi)
        pa = faces_ref[16 * m : 16 * m + 8, :]
        qa = faces_ref[16 * m + 8 : 16 * m + 16, :]
        ka = faces_ref[128 + m : 129 + m, :]
        i_s[0:1, cols] = cf_ref[0:1, cols]
        t_s[0:1, cols] = face_terms(pa, qa, ka, pb, qb, kb)[0]
    incoming(got, cells_ref, sc_ref, (6, 7), i_s, t_s, FX)
    gp_ref[...] = add_terms(i_s, t_s, 3, gpi_ref[...])
    gy_ref[:, :OWN] = gyi_ref[...]
    gy_ref[:, OWN:] = -y_ref[:, OWN:] * strain_of(s_ref, f_s, a_s)


def shape(*dims):
    return jax.ShapeDtypeStruct(dims, jnp.float32)


def on_device(
    displacement,
    adjoint_disp,
    pressure,
    adjoint_pressure,
    youngs,
    permeability,
    stiffness,
    send_nodes,
    send_cells,
    elem_nodes,
    inner_faces,
    cross_faces,
):
    forward = displacement.transpose(1, 0, 2)
    adjoint = adjoint_disp.transpose(1, 0, 2)
    perm = permeability.reshape(OWN_CHUNKS, LANES)
    young = youngs.reshape(1, EL)
    sources = (
        pressure,
        adjoint_pressure,
        perm,
        cross_faces,
        send_cells,
        send_nodes,
        forward,
        adjoint,
        elem_nodes,
        inner_faces,
        young,
        stiffness,
    )
    packed = pl.pallas_call(
        pack_kernel,
        out_shape=[shape(FAR_ROWS, LANES)]
        + [shape(ROWS, LANES)] * NEAR
        + [shape(24 * SLOTS, LANES), shape(144, LANES)]
        + [jax.ShapeDtypeStruct((48 * OWN_CHUNKS, 2 * LANES), jnp.bfloat16)]
        + [jax.ShapeDtypeStruct(one.shape, one.dtype) for one in sources],
        in_specs=[pl.BlockSpec(memory_space=pltpu.HBM)] * SOURCES,
        scratch_shapes=[pltpu.VMEM((48 * OWN_CHUNKS, LANES), jnp.float32), pltpu.SemaphoreType.DMA((SOURCES,))],
        compiler_params=VMEM,
        name="pack",
    )(*(pltpu.with_memory_space_constraint(one, pltpu.HBM) for one in sources))
    cells, faces, table = packed[NEAR + 1 : NEAR + 4]
    (
        pressure,
        adjoint_pressure,
        perm,
        cross_faces,
        send_cells,
        _,
        forward,
        adjoint,
        elem_nodes,
        inner_faces,
        young,
        stiffness,
    ) = packed[NEAR + 4 :]
    count = lax.axis_size("dom")
    swapped = lax.ppermute(packed[0], "dom", [(source, source ^ 8) for source in range(count)])
    near = []
    for number, j in enumerate(ORDER):
        pairs = [(source, (source - OFFSETS[j]) % count) for source in range(count)]
        near.append(lax.ppermute(packed[number + 1], "dom", pairs))
    inner_young, inner_perm = pl.pallas_call(
        inner_kernel,
        out_shape=[shape(1, EARLY), shape(OWN_CHUNKS, LANES)],
        scratch_shapes=[
            pltpu.VMEM((192, EARLY), jnp.float32),
            pltpu.VMEM((192, EARLY), jnp.float32),
            pltpu.VMEM((2, FI), jnp.float32),
        ],
        compiler_params=VMEM,
        cost_estimate=pl.CostEstimate(flops=4 * 10**9, bytes_accessed=10**7, transcendentals=0),
        name="inner",
    )(table, pressure, adjoint_pressure, perm, young, stiffness, elem_nodes, inner_faces)
    swapped, inner_young, inner_perm, table = lax.optimization_barrier((swapped, inner_young, inner_perm, table))
    relayed = lax.ppermute(
        swapped, "dom", [(source, (source - 16 if source & 8 else source + 16) % count) for source in range(count)]
    )
    own_young, edge_forward, edge_adjoint = pl.pallas_call(
        edge_kernel,
        out_shape=[shape(1, OWN), shape(192, EB), shape(192, EB)],
        scratch_shapes=[pltpu.VMEM((192, EB), jnp.float32), pltpu.VMEM((192, EB), jnp.float32)],
        compiler_params=VMEM,
        cost_estimate=pl.CostEstimate(flops=2 * 10**9, bytes_accessed=10**7, transcendentals=0),
        name="edge",
    )(table, forward, adjoint, young, stiffness, elem_nodes, inner_young)
    edge_forward, edge_adjoint, near_perm = pl.pallas_call(
        near_kernel,
        out_shape=[shape(192, EB), shape(192, EB), shape(OWN_CHUNKS, LANES)],
        scratch_shapes=[
            pltpu.VMEM((1, NEAR * FX), jnp.int32),
            pltpu.VMEM((1, NEAR * FX), jnp.float32),
            pltpu.VMEM((48 * NEAR, LANES), jnp.float32),
            pltpu.VMEM((48 * NEAR, 2 * LANES), jnp.bfloat16),
        ],
        compiler_params=VMEM,
        name="near",
    )(*near, edge_forward, edge_adjoint, cells, send_cells, elem_nodes, inner_perm)
    grad_young, grad_perm = pl.pallas_call(
        tail_kernel,
        out_shape=[shape(1, EL), shape(OWN_CHUNKS, LANES)],
        scratch_shapes=[
            pltpu.VMEM((192, EB), jnp.float32),
            pltpu.VMEM((192, EB), jnp.float32),
            pltpu.VMEM((1, 3 * FX), jnp.int32),
            pltpu.VMEM((1, 3 * FX), jnp.float32),
            pltpu.VMEM((96, LANES), jnp.float32),
            pltpu.VMEM((96, 2 * LANES), jnp.bfloat16),
            pltpu.VMEM((ROWS, LANES), jnp.float32),
            pltpu.VMEM((ROWS, LANES), jnp.float32),
        ],
        compiler_params=VMEM,
        name="tail",
    )(
        *near,
        swapped,
        relayed,
        edge_forward,
        edge_adjoint,
        cells,
        faces,
        young,
        stiffness,
        send_cells,
        elem_nodes,
        cross_faces,
        own_young,
        near_perm,
    )
    return (grad_young.reshape(EL), grad_perm.reshape(EL))


def solution(mesh):
    in_specs = (
        P(None, None, "dom"),
        P(None, None, "dom"),
        P(None, "dom"),
        P(None, "dom"),
        P("dom"),
        P("dom"),
        P(),
        P(None, "dom"),
        P(None, "dom"),
        P(None, "dom"),
        P(None, "dom"),
        P(None, "dom"),
    )
    out_specs = (P("dom"), P("dom"))
    return jax.shard_map(
        on_device, mesh=mesh, in_specs=in_specs, out_specs=out_specs, check_vma=False
    )
```

```python
import jax
import jax.numpy as jnp
from jax import lax
from jax.experimental import pallas as pl
from jax.experimental.pallas import tpu as pltpu
from jax.sharding import PartitionSpec as P


OFFSETS = (1, -1, 2, -2, 4, -4, 8, -8)
SLOTS = 8
STEPS = 8
EL = 2048
EB = 512
OWN = EL - EB
FI = 6144
FX = 1024
LANES = 128
OWN_CHUNKS = EL // LANES
NODE_ROWS = 6 * STEPS
FACE_ROW = NODE_ROWS + 24
FACE_K = FACE_ROW + 16 * (FX // LANES)
FACE_ID = FACE_K + 8
ROWS = FACE_ID + 8
VMEM = pltpu.CompilerParams(vmem_limit_bytes=48 * 2**20)


def lane_take(table, lo):
    return jnp.take_along_axis(table, lo, axis=1, mode="promise_in_bounds")


def split_index(row):
    wide = jnp.broadcast_to(row, (8, LANES))
    return wide & (LANES - 1), wide >> 7


def select_rows(tables, lo, hi, chunks):
    picked = [lane_take(table(0), lo) for table in tables]
    for chunk in range(1, chunks):
        here = hi == chunk
        picked = [jnp.where(here, lane_take(table(chunk), lo), old) for table, old in zip(tables, picked)]
    return picked


def select_scalar(blocks, lo, hi):
    sub = lax.broadcasted_iota(jnp.int32, (8, LANES), 0)
    total = None
    for number, block in enumerate(blocks):
        part = jnp.where(hi == sub + 8 * number, lane_take(block, lo), 0.0)
        total = part if total is None else total + part
    return jnp.sum(total, axis=0, keepdims=True)


def cell_tables(p_ref, q_ref):
    return [
        lambda h: p_ref[:, h * LANES : (h + 1) * LANES],
        lambda h: q_ref[:, h * LANES : (h + 1) * LANES],
    ]


def node_tables(d_ref, a_ref):
    def table(ref, comp):
        return lambda h: ref[comp, :, h * LANES : (h + 1) * LANES]

    return [table(d_ref, comp) for comp in range(3)] + [table(a_ref, comp) for comp in range(3)]


def face_terms(pa, qa, ka, pb, qb, kb):
    product = jnp.sum((pa - pb) * (qa - qb), axis=0, keepdims=True)
    total = ka + kb
    common = 2.0 * ka * kb * product / (total * total)
    return common * kb, common * ka


def scatter(index, term):
    length = index.shape[1]
    lo = index & (LANES - 1)
    hi = index >> 7
    hot = jnp.where(lax.broadcasted_iota(jnp.int32, (LANES, length), 0) == lo, 1.0, 0.0).astype(jnp.bfloat16)
    top = term.astype(jnp.bfloat16).astype(jnp.float32)
    rows = lax.broadcasted_iota(jnp.int32, (16, length), 0) == hi
    left = jnp.concatenate([jnp.where(rows, top, 0.0), jnp.where(rows, term - top, 0.0)], axis=0)
    out = lax.dot_general(
        left.astype(jnp.bfloat16), hot, (((1,), (1,)), ((), ())), preferred_element_type=jnp.float32
    )
    return out[:16] + out[16:]


def halves(value):
    top = value.astype(jnp.bfloat16)
    return top, (value - top.astype(jnp.float32)).astype(jnp.bfloat16)


def spread_stiffness(k_ref):
    pick = (
        lax.broadcasted_iota(jnp.int32, (192, 24), 0) // 8 == lax.broadcasted_iota(jnp.int32, (192, 24), 1)
    ).astype(jnp.float32).astype(jnp.bfloat16)
    same = (lax.broadcasted_iota(jnp.int32, (192, 192), 0) & 7) == (
        lax.broadcasted_iota(jnp.int32, (192, 192), 1) & 7
    )
    out = []
    for half in halves(k_ref[...]):
        tall = jnp.dot(pick, half, preferred_element_type=jnp.float32).astype(jnp.bfloat16)
        full = lax.dot_general(tall, pick, (((1,), (1,)), ((), ())), preferred_element_type=jnp.float32)
        out.append(jnp.where(same, full, 0.0).astype(jnp.bfloat16))
    return out


def strain_of(k_ref, f_ref, a_ref):
    top, low = spread_stiffness(k_ref)
    f_top, f_low = halves(f_ref[...])
    weighted = jnp.dot(top, f_top, preferred_element_type=jnp.float32)
    weighted += jnp.dot(low, f_top, preferred_element_type=jnp.float32)
    weighted += jnp.dot(top, f_low, preferred_element_type=jnp.float32)
    return jnp.sum(a_ref[...] * weighted, axis=0, keepdims=True)


def fill_table(raw_ref, tab_ref, chunks, read):
    for chunk in range(chunks):
        for number in range(6):
            line = 48 * chunk + 8 * number
            raw_ref[line : line + 8, :] = read(number, chunk)
    top, low = halves(raw_ref[...])
    tab_ref[:, :LANES] = top
    tab_ref[:, LANES:] = low


def lookup(tab_ref, rows, first, last, olds=(None, None)):
    sub = lax.broadcasted_iota(jnp.int32, (LANES, LANES), 0)
    hot = jnp.concatenate(
        [jnp.where(sub == (row & (LANES - 1)), 1.0, 0.0).astype(jnp.bfloat16) for row in rows], axis=1
    )
    found = jnp.dot(tab_ref[...], jnp.concatenate([hot, hot], axis=0), preferred_element_type=jnp.float32)
    results = []
    for place, (row, old) in enumerate(zip(rows, olds)):
        hi = jnp.broadcast_to(row >> 7, (8, LANES))
        got = [None] * 6 if old is None else old
        for chunk in range(first, last):
            base = 48 * (chunk - first)
            new = [found[base + 8 * r : base + 8 * r + 8, place * LANES : (place + 1) * LANES] for r in range(6)]
            here = hi == chunk
            got = [fresh if kept is None else jnp.where(here, fresh, kept) for fresh, kept in zip(new, got)]
        results.append(got)
    return results


def lines(corner):
    return [(8 * comp + corner) * 8 for comp in range(3)]


def put(f_ref, a_ref, corner, cols, got):
    for comp, line in enumerate(lines(corner)):
        f_ref[line : line + 8, cols] = got[comp]
        a_ref[line : line + 8, cols] = got[3 + comp]


def own_corners(tab_ref, nodes, elem, pairs, lone, f_ref, a_ref, cols):
    for pair in pairs:
        for corner, got in zip(pair, lookup(tab_ref, [elem[n : n + 1] for n in pair], 0, OWN_CHUNKS)):
            put(f_ref, a_ref, corner, cols, got)
    for corner in lone:
        lo, hi = split_index(elem[corner : corner + 1])
        put(f_ref, a_ref, corner, cols, select_rows(nodes, lo, hi, OWN_CHUNKS))


def ghost_corners(tab_ref, elem, first, last, old_f, old_a, f_ref, a_ref, cols, fresh):
    for pair in range(4):
        corners = (2 * pair, 2 * pair + 1)
        olds = [
            None
            if corner == 0 and fresh
            else [ref[line : line + 8, cols] for ref in (old_f, old_a) for line in lines(corner)]
            for corner in corners
        ]
        for corner, got in zip(corners, lookup(tab_ref, [elem[n : n + 1] for n in corners], first, last, olds)):
            put(f_ref, a_ref, corner, cols, got)


SOURCES = 12


def pack_kernel(*refs):
    sources, outs, (raw_s, sn_ref, sem) = refs[:SOURCES], refs[SOURCES:-3], refs[-3:]
    far_ref, near_refs, cells_ref, faces_ref = outs[0], outs[1 : NEAR + 1], outs[NEAR + 1], outs[NEAR + 2]
    tab_ref, local = outs[NEAR + 3], (*outs[NEAR + 4 :], sn_ref)
    copies = [pltpu.make_async_copy(far, near, sem.at[n]) for n, (far, near) in enumerate(zip(sources, local))]
    for copy in copies:
        copy.start()
    for copy in (*copies[:4], copies[-1]):
        copy.wait()
    p_ref, q_ref, k_ref, cf_ref, sc_ref, d_ref, a_ref = local[:7]
    nodes = node_tables(d_ref, a_ref)
    cells = cell_tables(p_ref, q_ref)
    perm = [k_ref[0:8, :], k_ref[8:16, :]]
    for m in range(FX // LANES):
        cols = slice(m * LANES, (m + 1) * LANES)
        lo, hi = split_index(cf_ref[0:1, cols])
        pa, qa = select_rows(cells, lo, hi, OWN_CHUNKS)
        ka = select_scalar(perm, lo, hi)
        slot = cf_ref[1:2, cols].astype(jnp.float32)
        for ref, base in [(one, FACE_ROW) for one in near_refs] + [(faces_ref, 0), (far_ref, FAR_FACES)]:
            ref[base + 16 * m : base + 16 * m + 8, :] = pa
            ref[base + 16 * m + 8 : base + 16 * m + 16, :] = qa
            ref[base + 128 + m : base + 129 + m, :] = ka
            ref[base + 136 + m : base + 137 + m, :] = slot
    for copy in copies[4:7]:
        copy.wait()
    fill_table(raw_s, tab_ref, OWN_CHUNKS, lambda number, chunk: nodes[number](chunk))
    for j in range(SLOTS):
        out, start = (near_refs[ORDER.index(j)], 0) if j < NEAR else (far_ref, BLOCK * (j - NEAR))
        if j % 2 == 0:
            both = lookup(tab_ref, [sn_ref[n : n + 1, :] for n in (j, j + 1)], 0, OWN_CHUNKS)
        for number, value in enumerate(both[j % 2]):
            out[start + 8 * number : start + 8 * number + 8, :] = value
        lo, hi = split_index(sc_ref[j : j + 1, :])
        pb, qb = select_rows(cells, lo, hi, OWN_CHUNKS)
        kb = jnp.broadcast_to(select_scalar(perm, lo, hi), (8, LANES))
        for ref, base in ((out, start + NODE_ROWS), (cells_ref, 24 * j)):
            ref[base : base + 8, :] = pb
            ref[base + 8 : base + 16, :] = qb
            ref[base + 16 : base + 24, :] = kb
    for copy in copies[7:-1]:
        copy.wait()


FACE_BLOCK = 6
EARLY = FI // FACE_BLOCK
ORDER = (2, 4, 0, 1, 5, 3)
NEAR = len(ORDER)
BLOCK = NODE_ROWS + 24
FAR_FACES = 2 * BLOCK
FAR_ROWS = FAR_FACES + 144


def inner_kernel(
    tab_ref, d_ref, a_ref, p_ref, q_ref, k_ref, y_ref, s_ref, en_ref, if_ref, gy_ref, gp_ref, fo_ref, ao_ref, f_s, a_s, t_s
):
    nodes = node_tables(d_ref, a_ref)
    cells = cell_tables(p_ref, q_ref)
    perm = [k_ref[0:8, :], k_ref[8:16, :]]
    width = FACE_BLOCK * LANES
    t_s[:, :width] = jnp.zeros((2, width), jnp.float32)

    def add(step, total):
        cols = pl.ds(pl.multiple_of(step * width, width), width)
        for side in range(2):
            total = total + scatter(if_ref[side : side + 1, cols], t_s[side : side + 1, cols])
        return total

    def block(step, total):
        total = add(jnp.maximum(step - 1, 0), total)
        cols = pl.ds(pl.multiple_of(step * LANES, LANES), LANES)
        elem = en_ref[:, cols]
        own_corners(tab_ref, None, elem, ((0, 1), (2, 3), (4, 5), (6, 7)), (), f_s, a_s, cols)
        for face in range(FACE_BLOCK):
            offset = pl.multiple_of(step * width + face * LANES, LANES)
            ends = []
            for side in range(2):
                lo, hi = split_index(if_ref[side : side + 1, pl.ds(offset, LANES)])
                ends += select_rows(cells, lo, hi, OWN_CHUNKS) + [select_scalar(perm, lo, hi)]
            term_a, term_b = face_terms(*ends)
            t_s[0:1, pl.ds(offset, LANES)] = term_a
            t_s[1:2, pl.ds(offset, LANES)] = term_b
        return total

    steps = FI // width
    total = lax.fori_loop(0, steps, block, jnp.zeros((16, LANES), jnp.float32))
    gp_ref[...] = add(steps - 1, total)

    def late(step, _):
        start = pl.multiple_of(step * LANES, LANES)
        place = pl.multiple_of(EARLY + start, LANES)
        elem = en_ref[:, pl.ds(place, LANES)]
        own_corners(tab_ref, nodes, elem, ((0, 1), (2, 3), (4, 5)), (6, 7), f_s, a_s, pl.ds(place, LANES))
        elem = en_ref[:, pl.ds(pl.multiple_of(OWN + start, LANES), LANES)]
        own_corners(tab_ref, nodes, elem, ((1, 2), (3, 4)), (5, 6, 7), fo_ref, ao_ref, pl.ds(start, LANES))
        return 0

    lax.fori_loop(0, EB // LANES, late, 0)
    gy_ref[...] = -y_ref[:, :OWN] * strain_of(s_ref, f_s, a_s)


def incoming(got, cells_ref, sc_ref, slots, i_s, t_s, start):
    for number, j in enumerate(slots):
        mine = j ^ 1
        pt = cells_ref[24 * mine : 24 * mine + 8, :]
        qt = cells_ref[24 * mine + 8 : 24 * mine + 16, :]
        kt = cells_ref[24 * mine + 16 : 24 * mine + 24, :]
        place = jnp.broadcast_to(sc_ref[mine : mine + 1, :], (8, LANES))
        for m in range(FX // LANES):
            base = start + number * FX + m * LANES
            cols = slice(base, base + LANES)
            lo, hi = split_index(got[j][FACE_ID + m : FACE_ID + m + 1, :].astype(jnp.int32))
            pa = got[j][FACE_ROW + 16 * m : FACE_ROW + 16 * m + 8, :]
            qa = got[j][FACE_ROW + 16 * m + 8 : FACE_ROW + 16 * m + 16, :]
            ka = got[j][FACE_K + m : FACE_K + m + 1, :]
            kb = lane_take(kt, lo)[0:1]
            term = face_terms(pa, qa, ka, lane_take(pt, lo), lane_take(qt, lo), kb)[1]
            i_s[0:1, cols] = lane_take(place, lo)[0:1]
            t_s[0:1, cols] = jnp.where(hi[0:1] == mine, term, 0.0)


def add_terms(i_s, t_s, count, total):
    def add(step, total):
        cols = pl.ds(pl.multiple_of(step * 1024, 1024), 1024)
        return total + scatter(i_s[0:1, cols], t_s[0:1, cols])

    return lax.fori_loop(0, count, add, total)


def tail_kernel(*refs):
    near, (swapped, relayed) = refs[:NEAR], refs[NEAR : NEAR + 2]
    (fo_ref, ao_ref, cells_ref, faces_ref, y_ref, s_ref, sc_ref, en_ref, cf_ref, gyi_ref, gpi_ref) = refs[NEAR + 2 : NEAR + 13]
    gy_ref, gp_ref, f_s, a_s, i_s, t_s, raw_s, tab_s, up_s, down_s = refs[NEAR + 13 :]
    got = [near[ORDER.index(j)] for j in range(NEAR)] + [up_s, down_s]
    low = jnp.broadcast_to((lax.axis_index("dom") & 8) == 0, (8, LANES))
    for ref, start, direct, other in ((up_s, 0, swapped, relayed), (down_s, BLOCK, relayed, swapped)):
        for to, source, length in ((0, start, BLOCK), (BLOCK, FAR_FACES, 144)):
            for row in range(0, length, 8):
                ref[to + row : to + row + 8, :] = jnp.where(
                    low, direct[source + row : source + row + 8, :], other[source + row : source + row + 8, :]
                )
    fill_table(raw_s, tab_s, SLOTS, lambda number, chunk: got[chunk][8 * number : 8 * number + 8, :])
    for step in range(EB // LANES):
        elem = en_ref[:, OWN + step * LANES : OWN + (step + 1) * LANES]
        cols = slice(step * LANES, (step + 1) * LANES)
        ghost_corners(tab_s, elem, OWN_CHUNKS, OWN_CHUNKS + SLOTS, fo_ref, ao_ref, f_s, a_s, cols, True)

    ghosts = [
        lambda h: got[h][NODE_ROWS : NODE_ROWS + 8, :],
        lambda h: got[h][NODE_ROWS + 8 : NODE_ROWS + 16, :],
    ]
    ghost_perm = jnp.concatenate([got[j][NODE_ROWS + 16 : NODE_ROWS + 17, :] for j in range(SLOTS)], axis=0)
    for m in range(FX // LANES):
        cols = slice(m * LANES, (m + 1) * LANES)
        lo, hi = split_index(cf_ref[1:2, cols])
        pb, qb = select_rows(ghosts, lo, hi, SLOTS)
        kb = select_scalar([ghost_perm], lo, hi)
        pa = faces_ref[16 * m : 16 * m + 8, :]
        qa = faces_ref[16 * m + 8 : 16 * m + 16, :]
        ka = faces_ref[128 + m : 129 + m, :]
        i_s[0:1, cols] = cf_ref[0:1, cols]
        t_s[0:1, cols] = face_terms(pa, qa, ka, pb, qb, kb)[0]
    incoming(got, cells_ref, sc_ref, range(SLOTS), i_s, t_s, FX)
    gp_ref[...] = add_terms(i_s, t_s, SLOTS + 1, gpi_ref[...])
    gy_ref[:, :OWN] = gyi_ref[...]
    gy_ref[:, OWN:] = -y_ref[:, OWN:] * strain_of(s_ref, f_s, a_s)


def shape(*dims):
    return jax.ShapeDtypeStruct(dims, jnp.float32)


def on_device(
    displacement,
    adjoint_disp,
    pressure,
    adjoint_pressure,
    youngs,
    permeability,
    stiffness,
    send_nodes,
    send_cells,
    elem_nodes,
    inner_faces,
    cross_faces,
):
    forward = displacement.transpose(1, 0, 2)
    adjoint = adjoint_disp.transpose(1, 0, 2)
    perm = permeability.reshape(OWN_CHUNKS, LANES)
    young = youngs.reshape(1, EL)
    sources = (
        pressure,
        adjoint_pressure,
        perm,
        cross_faces,
        send_cells,
        forward,
        adjoint,
        elem_nodes,
        inner_faces,
        young,
        stiffness,
        send_nodes,
    )
    packed = pl.pallas_call(
        pack_kernel,
        out_shape=[shape(FAR_ROWS, LANES)]
        + [shape(ROWS, LANES)] * NEAR
        + [shape(24 * SLOTS, LANES), shape(144, LANES)]
        + [jax.ShapeDtypeStruct((48 * OWN_CHUNKS, 2 * LANES), jnp.bfloat16)]
        + [jax.ShapeDtypeStruct(one.shape, one.dtype) for one in sources[:-1]],
        in_specs=[pl.BlockSpec(memory_space=pltpu.HBM)] * SOURCES,
        scratch_shapes=[
            pltpu.VMEM((48 * OWN_CHUNKS, LANES), jnp.float32),
            pltpu.VMEM((SLOTS, LANES), jnp.int32),
            pltpu.SemaphoreType.DMA((SOURCES,)),
        ],
        compiler_params=VMEM,
        name="pack",
    )(*(pltpu.with_memory_space_constraint(one, pltpu.HBM) for one in sources))
    cells, faces, table = packed[NEAR + 1 : NEAR + 4]
    (
        pressure,
        adjoint_pressure,
        perm,
        cross_faces,
        send_cells,
        forward,
        adjoint,
        elem_nodes,
        inner_faces,
        young,
        stiffness,
    ) = packed[NEAR + 4 :]
    count = lax.axis_size("dom")
    swapped = lax.ppermute(packed[0], "dom", [(source, source ^ 8) for source in range(count)])
    near = []
    for number, j in enumerate(ORDER):
        pairs = [(source, (source - OFFSETS[j]) % count) for source in range(count)]
        near.append(lax.ppermute(packed[number + 1], "dom", pairs))
    relayed = lax.ppermute(
        swapped, "dom", [(source, (source - 16 if source & 8 else source + 16) % count) for source in range(count)]
    )
    own_young, own_perm, edge_forward, edge_adjoint = pl.pallas_call(
        inner_kernel,
        out_shape=[shape(1, OWN), shape(OWN_CHUNKS, LANES), shape(192, EB), shape(192, EB)],
        scratch_shapes=[
            pltpu.VMEM((192, OWN), jnp.float32),
            pltpu.VMEM((192, OWN), jnp.float32),
            pltpu.VMEM((2, FI), jnp.float32),
        ],
        compiler_params=VMEM,
        cost_estimate=pl.CostEstimate(flops=4 * 10**9, bytes_accessed=10**7, transcendentals=0),
        name="inner",
    )(table, forward, adjoint, pressure, adjoint_pressure, perm, young, stiffness, elem_nodes, inner_faces)
    grad_young, grad_perm = pl.pallas_call(
        tail_kernel,
        out_shape=[shape(1, EL), shape(OWN_CHUNKS, LANES)],
        scratch_shapes=[
            pltpu.VMEM((192, EB), jnp.float32),
            pltpu.VMEM((192, EB), jnp.float32),
            pltpu.VMEM((1, (SLOTS + 1) * FX), jnp.int32),
            pltpu.VMEM((1, (SLOTS + 1) * FX), jnp.float32),
            pltpu.VMEM((48 * SLOTS, LANES), jnp.float32),
            pltpu.VMEM((48 * SLOTS, 2 * LANES), jnp.bfloat16),
            pltpu.VMEM((ROWS, LANES), jnp.float32),
            pltpu.VMEM((ROWS, LANES), jnp.float32),
        ],
        compiler_params=VMEM,
        name="tail",
    )(
        *near,
        swapped,
        relayed,
        edge_forward,
        edge_adjoint,
        cells,
        faces,
        young,
        stiffness,
        send_cells,
        elem_nodes,
        cross_faces,
        own_young,
        own_perm,
    )
    return (grad_young.reshape(EL), grad_perm.reshape(EL))


def solution(mesh):
    in_specs = (
        P(None, None, "dom"),
        P(None, None, "dom"),
        P(None, "dom"),
        P(None, "dom"),
        P("dom"),
        P("dom"),
        P(),
        P(None, "dom"),
        P(None, "dom"),
        P(None, "dom"),
        P(None, "dom"),
        P(None, "dom"),
    )
    out_specs = (P("dom"), P("dom"))
    return jax.shard_map(
        on_device, mesh=mesh, in_specs=in_specs, out_specs=out_specs, check_vma=False
    )
```

```python
import jax
import jax.numpy as jnp
from jax import lax
from jax.experimental import pallas as pl
from jax.experimental.pallas import tpu as pltpu
from jax.sharding import PartitionSpec as P


OFFSETS = (1, -1, 2, -2, 4, -4, 8, -8)
SLOTS = 8
STEPS = 8
EL = 2048
EB = 512
OWN = EL - EB
FI = 6144
FX = 1024
LANES = 128
OWN_CHUNKS = EL // LANES
NODE_ROWS = 6 * STEPS
FACE_ROW = NODE_ROWS + 24
FACE_K = FACE_ROW + 16 * (FX // LANES)
FACE_ID = FACE_K + 8
ROWS = FACE_ID + 8
VMEM = pltpu.CompilerParams(vmem_limit_bytes=48 * 2**20)


def lane_take(table, lo):
    return jnp.take_along_axis(table, lo, axis=1, mode="promise_in_bounds")


def split_index(row):
    wide = jnp.broadcast_to(row, (8, LANES))
    return wide & (LANES - 1), wide >> 7


def select_rows(tables, lo, hi, chunks):
    picked = [lane_take(table(0), lo) for table in tables]
    for chunk in range(1, chunks):
        here = hi == chunk
        picked = [jnp.where(here, lane_take(table(chunk), lo), old) for table, old in zip(tables, picked)]
    return picked


def select_scalar(blocks, lo, hi):
    sub = lax.broadcasted_iota(jnp.int32, (8, LANES), 0)
    total = None
    for number, block in enumerate(blocks):
        part = jnp.where(hi == sub + 8 * number, lane_take(block, lo), 0.0)
        total = part if total is None else total + part
    return jnp.sum(total, axis=0, keepdims=True)


def cell_tables(p_ref, q_ref):
    return [
        lambda h: p_ref[:, h * LANES : (h + 1) * LANES],
        lambda h: q_ref[:, h * LANES : (h + 1) * LANES],
    ]


def node_tables(d_ref, a_ref):
    def table(ref, comp):
        return lambda h: ref[comp, :, h * LANES : (h + 1) * LANES]

    return [table(d_ref, comp) for comp in range(3)] + [table(a_ref, comp) for comp in range(3)]


def face_terms(pa, qa, ka, pb, qb, kb):
    product = jnp.sum((pa - pb) * (qa - qb), axis=0, keepdims=True)
    total = ka + kb
    common = 2.0 * ka * kb * product / (total * total)
    return common * kb, common * ka


def one_hot(lo):
    rows = lax.broadcasted_iota(jnp.int32, (LANES, lo.shape[1]), 0).astype(jnp.float32).astype(jnp.bfloat16)
    here = rows == lo.astype(jnp.float32).astype(jnp.bfloat16)
    return jnp.where(here, jnp.bfloat16(1), jnp.bfloat16(0))


def scatter(index, term):
    length = index.shape[1]
    lo = index & (LANES - 1)
    hi = index >> 7
    hot = one_hot(lo)
    top = term.astype(jnp.bfloat16).astype(jnp.float32)
    rows = lax.broadcasted_iota(jnp.int32, (16, length), 0) == hi
    left = jnp.concatenate([jnp.where(rows, top, 0.0), jnp.where(rows, term - top, 0.0)], axis=0)
    out = lax.dot_general(
        left.astype(jnp.bfloat16), hot, (((1,), (1,)), ((), ())), preferred_element_type=jnp.float32
    )
    return out[:16] + out[16:]


def halves(value):
    top = value.astype(jnp.bfloat16)
    return top, (value - top.astype(jnp.float32)).astype(jnp.bfloat16)


def spread_stiffness(k_ref):
    pick = (
        lax.broadcasted_iota(jnp.int32, (192, 24), 0) // 8 == lax.broadcasted_iota(jnp.int32, (192, 24), 1)
    ).astype(jnp.float32).astype(jnp.bfloat16)
    same = (lax.broadcasted_iota(jnp.int32, (192, 192), 0) & 7) == (
        lax.broadcasted_iota(jnp.int32, (192, 192), 1) & 7
    )
    out = []
    for half in halves(k_ref[...]):
        tall = jnp.dot(pick, half, preferred_element_type=jnp.float32).astype(jnp.bfloat16)
        full = lax.dot_general(tall, pick, (((1,), (1,)), ((), ())), preferred_element_type=jnp.float32)
        out.append(jnp.where(same, full, 0.0).astype(jnp.bfloat16))
    return out


def strain_of(k_ref, f_ref, a_ref):
    top, low = spread_stiffness(k_ref)
    f_top, f_low = halves(f_ref[...])
    weighted = jnp.dot(top, f_top, preferred_element_type=jnp.float32)
    weighted += jnp.dot(low, f_top, preferred_element_type=jnp.float32)
    weighted += jnp.dot(top, f_low, preferred_element_type=jnp.float32)
    return jnp.sum(a_ref[...] * weighted, axis=0, keepdims=True)


def fill_table(raw_ref, tab_ref, chunks, read):
    for chunk in range(chunks):
        for number in range(6):
            line = 48 * chunk + 8 * number
            raw_ref[line : line + 8, :] = read(number, chunk)
    top, low = halves(raw_ref[...])
    tab_ref[:, :LANES] = top
    tab_ref[:, LANES:] = low


def lookup(tab_ref, rows, first, last, olds=(None, None)):
    hot = jnp.concatenate([one_hot(row & (LANES - 1)) for row in rows], axis=1)
    found = jnp.dot(tab_ref[...], jnp.concatenate([hot, hot], axis=0), preferred_element_type=jnp.float32)
    results = []
    for place, (row, old) in enumerate(zip(rows, olds)):
        hi = jnp.broadcast_to(row >> 7, (8, LANES))
        got = [None] * 6 if old is None else old
        for chunk in range(first, last):
            base = 48 * (chunk - first)
            new = [found[base + 8 * r : base + 8 * r + 8, place * LANES : (place + 1) * LANES] for r in range(6)]
            here = hi == chunk
            got = [fresh if kept is None else jnp.where(here, fresh, kept) for fresh, kept in zip(new, got)]
        results.append(got)
    return results


def lines(corner):
    return [(8 * comp + corner) * 8 for comp in range(3)]


def put(f_ref, a_ref, corner, cols, got):
    for comp, line in enumerate(lines(corner)):
        f_ref[line : line + 8, cols] = got[comp]
        a_ref[line : line + 8, cols] = got[3 + comp]


def own_corners(tab_ref, nodes, elem, pairs, lone, f_ref, a_ref, cols):
    for pair in pairs:
        for corner, got in zip(pair, lookup(tab_ref, [elem[n : n + 1] for n in pair], 0, OWN_CHUNKS)):
            put(f_ref, a_ref, corner, cols, got)
    for corner in lone:
        lo, hi = split_index(elem[corner : corner + 1])
        put(f_ref, a_ref, corner, cols, select_rows(nodes, lo, hi, OWN_CHUNKS))


def ghost_corners(tab_ref, elem, first, last, old_f, old_a, f_ref, a_ref, cols, fresh):
    for pair in range(4):
        corners = (2 * pair, 2 * pair + 1)
        olds = [
            None
            if corner == 0 and fresh
            else [ref[line : line + 8, cols] for ref in (old_f, old_a) for line in lines(corner)]
            for corner in corners
        ]
        for corner, got in zip(corners, lookup(tab_ref, [elem[n : n + 1] for n in corners], first, last, olds)):
            put(f_ref, a_ref, corner, cols, got)


SOURCES = 12


def pack_kernel(*refs):
    sources, outs, (raw_s, sn_ref, sem) = refs[:SOURCES], refs[SOURCES:-3], refs[-3:]
    far_ref, near_refs, cells_ref, faces_ref = outs[0], outs[1 : NEAR + 1], outs[NEAR + 1], outs[NEAR + 2]
    tab_ref, local = outs[NEAR + 3], (*outs[NEAR + 4 :], sn_ref)
    copies = [pltpu.make_async_copy(far, near, sem.at[n]) for n, (far, near) in enumerate(zip(sources, local))]
    for copy in copies:
        copy.start()
    for copy in (*copies[:4], copies[-1]):
        copy.wait()
    p_ref, q_ref, k_ref, cf_ref, sc_ref, d_ref, a_ref = local[:7]
    nodes = node_tables(d_ref, a_ref)
    cells = cell_tables(p_ref, q_ref)
    perm = [k_ref[0:8, :], k_ref[8:16, :]]
    for m in range(FX // LANES):
        cols = slice(m * LANES, (m + 1) * LANES)
        lo, hi = split_index(cf_ref[0:1, cols])
        pa, qa = select_rows(cells, lo, hi, OWN_CHUNKS)
        ka = select_scalar(perm, lo, hi)
        slot = cf_ref[1:2, cols].astype(jnp.float32)
        for ref, base in [(one, FACE_ROW) for one in near_refs] + [(faces_ref, 0), (far_ref, FAR_FACES)]:
            ref[base + 16 * m : base + 16 * m + 8, :] = pa
            ref[base + 16 * m + 8 : base + 16 * m + 16, :] = qa
            ref[base + 128 + m : base + 129 + m, :] = ka
            ref[base + 136 + m : base + 137 + m, :] = slot
    for copy in copies[4:7]:
        copy.wait()
    fill_table(raw_s, tab_ref, OWN_CHUNKS, lambda number, chunk: nodes[number](chunk))
    for j in range(SLOTS):
        out, start = (near_refs[ORDER.index(j)], 0) if j < NEAR else (far_ref, BLOCK * (j - NEAR))
        if j % 2 == 0:
            both = lookup(tab_ref, [sn_ref[n : n + 1, :] for n in (j, j + 1)], 0, OWN_CHUNKS)
        for number, value in enumerate(both[j % 2]):
            out[start + 8 * number : start + 8 * number + 8, :] = value
        lo, hi = split_index(sc_ref[j : j + 1, :])
        pb, qb = select_rows(cells, lo, hi, OWN_CHUNKS)
        kb = jnp.broadcast_to(select_scalar(perm, lo, hi), (8, LANES))
        for ref, base in ((out, start + NODE_ROWS), (cells_ref, 24 * j)):
            ref[base : base + 8, :] = pb
            ref[base + 8 : base + 16, :] = qb
            ref[base + 16 : base + 24, :] = kb
    for copy in copies[7:-1]:
        copy.wait()


FACE_BLOCK = 6
EARLY = FI // FACE_BLOCK
ORDER = (3, 5, 1, 0, 4, 2)
NEAR = len(ORDER)
BLOCK = NODE_ROWS + 24
FAR_FACES = 2 * BLOCK
FAR_ROWS = FAR_FACES + 144


def inner_kernel(
    tab_ref, d_ref, a_ref, p_ref, q_ref, k_ref, y_ref, s_ref, en_ref, if_ref, gy_ref, gp_ref, fo_ref, ao_ref, f_s, a_s, t_s
):
    nodes = node_tables(d_ref, a_ref)
    cells = cell_tables(p_ref, q_ref)
    perm = [k_ref[0:8, :], k_ref[8:16, :]]
    width = FACE_BLOCK * LANES
    t_s[:, :width] = jnp.zeros((2, width), jnp.float32)

    def add(step, total):
        cols = pl.ds(pl.multiple_of(step * width, width), width)
        for side in range(2):
            total = total + scatter(if_ref[side : side + 1, cols], t_s[side : side + 1, cols])
        return total

    def block(step, total):
        total = add(jnp.maximum(step - 1, 0), total)
        cols = pl.ds(pl.multiple_of(step * LANES, LANES), LANES)
        elem = en_ref[:, cols]
        own_corners(tab_ref, None, elem, ((0, 1), (2, 3), (4, 5), (6, 7)), (), f_s, a_s, cols)
        for face in range(FACE_BLOCK):
            offset = pl.multiple_of(step * width + face * LANES, LANES)
            ends = []
            for side in range(2):
                lo, hi = split_index(if_ref[side : side + 1, pl.ds(offset, LANES)])
                ends += select_rows(cells, lo, hi, OWN_CHUNKS) + [select_scalar(perm, lo, hi)]
            term_a, term_b = face_terms(*ends)
            t_s[0:1, pl.ds(offset, LANES)] = term_a
            t_s[1:2, pl.ds(offset, LANES)] = term_b
        return total

    steps = FI // width
    total = lax.fori_loop(0, steps, block, jnp.zeros((16, LANES), jnp.float32))
    gp_ref[...] = add(steps - 1, total)

    def late(step, _):
        start = pl.multiple_of(step * LANES, LANES)
        place = pl.multiple_of(EARLY + start, LANES)
        elem = en_ref[:, pl.ds(place, LANES)]
        own_corners(tab_ref, nodes, elem, ((0, 1), (2, 3), (4, 5)), (6, 7), f_s, a_s, pl.ds(place, LANES))
        elem = en_ref[:, pl.ds(pl.multiple_of(OWN + start, LANES), LANES)]
        own_corners(tab_ref, nodes, elem, ((1, 2), (3, 4)), (5, 6, 7), fo_ref, ao_ref, pl.ds(start, LANES))
        return 0

    lax.fori_loop(0, EB // LANES, late, 0)
    gy_ref[...] = -y_ref[:, :OWN] * strain_of(s_ref, f_s, a_s)


def incoming(got, cells_ref, sc_ref, slots, i_s, t_s, start):
    for number, j in enumerate(slots):
        mine = j ^ 1
        pt = cells_ref[24 * mine : 24 * mine + 8, :]
        qt = cells_ref[24 * mine + 8 : 24 * mine + 16, :]
        kt = cells_ref[24 * mine + 16 : 24 * mine + 24, :]
        place = jnp.broadcast_to(sc_ref[mine : mine + 1, :], (8, LANES))
        for m in range(FX // LANES):
            base = start + number * FX + m * LANES
            cols = slice(base, base + LANES)
            lo, hi = split_index(got[j][FACE_ID + m : FACE_ID + m + 1, :].astype(jnp.int32))
            pa = got[j][FACE_ROW + 16 * m : FACE_ROW + 16 * m + 8, :]
            qa = got[j][FACE_ROW + 16 * m + 8 : FACE_ROW + 16 * m + 16, :]
            ka = got[j][FACE_K + m : FACE_K + m + 1, :]
            kb = lane_take(kt, lo)[0:1]
            term = face_terms(pa, qa, ka, lane_take(pt, lo), lane_take(qt, lo), kb)[1]
            i_s[0:1, cols] = lane_take(place, lo)[0:1]
            t_s[0:1, cols] = jnp.where(hi[0:1] == mine, term, 0.0)


def add_terms(i_s, t_s, count, total):
    def add(step, total):
        cols = pl.ds(pl.multiple_of(step * 1024, 1024), 1024)
        return total + scatter(i_s[0:1, cols], t_s[0:1, cols])

    return lax.fori_loop(0, count, add, total)


def tail_kernel(*refs):
    near, (swapped, relayed) = refs[:NEAR], refs[NEAR : NEAR + 2]
    (fo_ref, ao_ref, cells_ref, faces_ref, y_ref, s_ref, sc_ref, en_ref, cf_ref, gyi_ref, gpi_ref) = refs[NEAR + 2 : NEAR + 13]
    gy_ref, gp_ref, f_s, a_s, i_s, t_s, raw_s, tab_s, up_s, down_s = refs[NEAR + 13 :]
    got = [near[ORDER.index(j)] for j in range(NEAR)] + [up_s, down_s]
    low = jnp.broadcast_to((lax.axis_index("dom") & 8) == 0, (8, LANES))
    for ref, start, direct, other in ((up_s, 0, swapped, relayed), (down_s, BLOCK, relayed, swapped)):
        for to, source, length in ((0, start, BLOCK), (BLOCK, FAR_FACES, 144)):
            for row in range(0, length, 8):
                ref[to + row : to + row + 8, :] = jnp.where(
                    low, direct[source + row : source + row + 8, :], other[source + row : source + row + 8, :]
                )
    fill_table(raw_s, tab_s, SLOTS, lambda number, chunk: got[chunk][8 * number : 8 * number + 8, :])
    for step in range(EB // LANES):
        elem = en_ref[:, OWN + step * LANES : OWN + (step + 1) * LANES]
        cols = slice(step * LANES, (step + 1) * LANES)
        ghost_corners(tab_s, elem, OWN_CHUNKS, OWN_CHUNKS + SLOTS, fo_ref, ao_ref, f_s, a_s, cols, True)

    ghosts = [
        lambda h: got[h][NODE_ROWS : NODE_ROWS + 8, :],
        lambda h: got[h][NODE_ROWS + 8 : NODE_ROWS + 16, :],
    ]
    ghost_perm = jnp.concatenate([got[j][NODE_ROWS + 16 : NODE_ROWS + 17, :] for j in range(SLOTS)], axis=0)
    for m in range(FX // LANES):
        cols = slice(m * LANES, (m + 1) * LANES)
        lo, hi = split_index(cf_ref[1:2, cols])
        pb, qb = select_rows(ghosts, lo, hi, SLOTS)
        kb = select_scalar([ghost_perm], lo, hi)
        pa = faces_ref[16 * m : 16 * m + 8, :]
        qa = faces_ref[16 * m + 8 : 16 * m + 16, :]
        ka = faces_ref[128 + m : 129 + m, :]
        i_s[0:1, cols] = cf_ref[0:1, cols]
        t_s[0:1, cols] = face_terms(pa, qa, ka, pb, qb, kb)[0]
    incoming(got, cells_ref, sc_ref, range(SLOTS), i_s, t_s, FX)
    gp_ref[...] = add_terms(i_s, t_s, SLOTS + 1, gpi_ref[...])
    gy_ref[:, :OWN] = gyi_ref[...]
    gy_ref[:, OWN:] = -y_ref[:, OWN:] * strain_of(s_ref, f_s, a_s)


def shape(*dims):
    return jax.ShapeDtypeStruct(dims, jnp.float32)


def on_device(
    displacement,
    adjoint_disp,
    pressure,
    adjoint_pressure,
    youngs,
    permeability,
    stiffness,
    send_nodes,
    send_cells,
    elem_nodes,
    inner_faces,
    cross_faces,
):
    forward = displacement.transpose(1, 0, 2)
    adjoint = adjoint_disp.transpose(1, 0, 2)
    perm = permeability.reshape(OWN_CHUNKS, LANES)
    young = youngs.reshape(1, EL)
    sources = (
        pressure,
        adjoint_pressure,
        perm,
        cross_faces,
        send_cells,
        forward,
        adjoint,
        elem_nodes,
        inner_faces,
        young,
        stiffness,
        send_nodes,
    )
    packed = pl.pallas_call(
        pack_kernel,
        out_shape=[shape(FAR_ROWS, LANES)]
        + [shape(ROWS, LANES)] * NEAR
        + [shape(24 * SLOTS, LANES), shape(144, LANES)]
        + [jax.ShapeDtypeStruct((48 * OWN_CHUNKS, 2 * LANES), jnp.bfloat16)]
        + [jax.ShapeDtypeStruct(one.shape, one.dtype) for one in sources[:-1]],
        in_specs=[pl.BlockSpec(memory_space=pltpu.HBM)] * SOURCES,
        scratch_shapes=[
            pltpu.VMEM((48 * OWN_CHUNKS, LANES), jnp.float32),
            pltpu.VMEM((SLOTS, LANES), jnp.int32),
            pltpu.SemaphoreType.DMA((SOURCES,)),
        ],
        compiler_params=VMEM,
        name="pack",
    )(*(pltpu.with_memory_space_constraint(one, pltpu.HBM) for one in sources))
    cells, faces, table = packed[NEAR + 1 : NEAR + 4]
    (
        pressure,
        adjoint_pressure,
        perm,
        cross_faces,
        send_cells,
        forward,
        adjoint,
        elem_nodes,
        inner_faces,
        young,
        stiffness,
    ) = packed[NEAR + 4 :]
    count = lax.axis_size("dom")
    swapped = lax.ppermute(packed[0], "dom", [(source, source ^ 8) for source in range(count)])
    near = []
    for number, j in enumerate(ORDER):
        pairs = [(source, (source - OFFSETS[j]) % count) for source in range(count)]
        near.append(lax.ppermute(packed[number + 1], "dom", pairs))
    relayed = lax.ppermute(
        swapped, "dom", [(source, (source - 16 if source & 8 else source + 16) % count) for source in range(count)]
    )
    own_young, own_perm, edge_forward, edge_adjoint = pl.pallas_call(
        inner_kernel,
        out_shape=[shape(1, OWN), shape(OWN_CHUNKS, LANES), shape(192, EB), shape(192, EB)],
        scratch_shapes=[
            pltpu.VMEM((192, OWN), jnp.float32),
            pltpu.VMEM((192, OWN), jnp.float32),
            pltpu.VMEM((2, FI), jnp.float32),
        ],
        compiler_params=VMEM,
        cost_estimate=pl.CostEstimate(flops=4 * 10**9, bytes_accessed=10**7, transcendentals=0),
        name="inner",
    )(table, forward, adjoint, pressure, adjoint_pressure, perm, young, stiffness, elem_nodes, inner_faces)
    grad_young, grad_perm = pl.pallas_call(
        tail_kernel,
        out_shape=[shape(1, EL), shape(OWN_CHUNKS, LANES)],
        scratch_shapes=[
            pltpu.VMEM((192, EB), jnp.float32),
            pltpu.VMEM((192, EB), jnp.float32),
            pltpu.VMEM((1, (SLOTS + 1) * FX), jnp.int32),
            pltpu.VMEM((1, (SLOTS + 1) * FX), jnp.float32),
            pltpu.VMEM((48 * SLOTS, LANES), jnp.float32),
            pltpu.VMEM((48 * SLOTS, 2 * LANES), jnp.bfloat16),
            pltpu.VMEM((ROWS, LANES), jnp.float32),
            pltpu.VMEM((ROWS, LANES), jnp.float32),
        ],
        compiler_params=VMEM,
        name="tail",
    )(
        *near,
        swapped,
        relayed,
        edge_forward,
        edge_adjoint,
        cells,
        faces,
        young,
        stiffness,
        send_cells,
        elem_nodes,
        cross_faces,
        own_young,
        own_perm,
    )
    return (grad_young.reshape(EL), grad_perm.reshape(EL))


def solution(mesh):
    in_specs = (
        P(None, None, "dom"),
        P(None, None, "dom"),
        P(None, "dom"),
        P(None, "dom"),
        P("dom"),
        P("dom"),
        P(),
        P(None, "dom"),
        P(None, "dom"),
        P(None, "dom"),
        P(None, "dom"),
        P(None, "dom"),
    )
    out_specs = (P("dom"), P("dom"))
    return jax.shard_map(
        on_device, mesh=mesh, in_specs=in_specs, out_specs=out_specs, check_vma=False
    )
```

```python
import jax
import jax.numpy as jnp
from jax import lax
from jax.experimental import pallas as pl
from jax.experimental.pallas import tpu as pltpu
from jax.sharding import PartitionSpec as P


OFFSETS = (1, -1, 2, -2, 4, -4, 8, -8)
SLOTS = 8
STEPS = 8
EL = 2048
EB = 512
OWN = EL - EB
FI = 6144
FX = 1024
LANES = 128
OWN_CHUNKS = EL // LANES
NODE_ROWS = 6 * STEPS
FACE_ROW = NODE_ROWS + 24
FACE_K = FACE_ROW + 16 * (FX // LANES)
FACE_ID = FACE_K + 8
ROWS = FACE_ID + 8
VMEM = pltpu.CompilerParams(vmem_limit_bytes=48 * 2**20)


def lane_take(table, lo):
    return jnp.take_along_axis(table, lo, axis=1, mode="promise_in_bounds")


def split_index(row):
    wide = jnp.broadcast_to(row, (8, LANES))
    return wide & (LANES - 1), wide >> 7


def select_rows(tables, lo, hi, chunks):
    picked = [lane_take(table(0), lo) for table in tables]
    for chunk in range(1, chunks):
        here = hi == chunk
        picked = [jnp.where(here, lane_take(table(chunk), lo), old) for table, old in zip(tables, picked)]
    return picked


def select_scalar(blocks, lo, hi):
    sub = lax.broadcasted_iota(jnp.int32, (8, LANES), 0)
    total = None
    for number, block in enumerate(blocks):
        part = jnp.where(hi == sub + 8 * number, lane_take(block, lo), 0.0)
        total = part if total is None else total + part
    return jnp.sum(total, axis=0, keepdims=True)


def cell_tables(p_ref, q_ref):
    return [
        lambda h: p_ref[:, h * LANES : (h + 1) * LANES],
        lambda h: q_ref[:, h * LANES : (h + 1) * LANES],
    ]


def node_tables(d_ref, a_ref):
    def table(ref, comp):
        return lambda h: ref[comp, :, h * LANES : (h + 1) * LANES]

    return [table(d_ref, comp) for comp in range(3)] + [table(a_ref, comp) for comp in range(3)]


def face_terms(pa, qa, ka, pb, qb, kb):
    product = jnp.sum((pa - pb) * (qa - qb), axis=0, keepdims=True)
    total = ka + kb
    common = 2.0 * ka * kb * product / (total * total)
    return common * kb, common * ka


def one_hot(lo):
    rows = lax.broadcasted_iota(jnp.int32, (LANES, lo.shape[1]), 0).astype(jnp.float32).astype(jnp.bfloat16)
    here = rows == lo.astype(jnp.float32).astype(jnp.bfloat16)
    return jnp.where(here, jnp.bfloat16(1), jnp.bfloat16(0))


def scatter(index, term):
    length = index.shape[1]
    lo = index & (LANES - 1)
    hi = index >> 7
    hot = one_hot(lo)
    top = term.astype(jnp.bfloat16).astype(jnp.float32)
    rows = lax.broadcasted_iota(jnp.int32, (16, length), 0) == hi
    left = jnp.concatenate([jnp.where(rows, top, 0.0), jnp.where(rows, term - top, 0.0)], axis=0)
    out = lax.dot_general(
        left.astype(jnp.bfloat16), hot, (((1,), (1,)), ((), ())), preferred_element_type=jnp.float32
    )
    return out[:16] + out[16:]


def halves(value):
    top = value.astype(jnp.bfloat16)
    return top, (value - top.astype(jnp.float32)).astype(jnp.bfloat16)


def spread_stiffness(k_ref):
    pick = (
        lax.broadcasted_iota(jnp.int32, (192, 24), 0) // 8 == lax.broadcasted_iota(jnp.int32, (192, 24), 1)
    ).astype(jnp.float32).astype(jnp.bfloat16)
    same = (lax.broadcasted_iota(jnp.int32, (192, 192), 0) & 7) == (
        lax.broadcasted_iota(jnp.int32, (192, 192), 1) & 7
    )
    out = []
    for half in halves(k_ref[...]):
        tall = jnp.dot(pick, half, preferred_element_type=jnp.float32).astype(jnp.bfloat16)
        full = lax.dot_general(tall, pick, (((1,), (1,)), ((), ())), preferred_element_type=jnp.float32)
        out.append(jnp.where(same, full, 0.0).astype(jnp.bfloat16))
    return out


def strain_of(k_ref, f_ref, a_ref):
    top, low = spread_stiffness(k_ref)
    f_top, f_low = halves(f_ref[...])
    weighted = jnp.dot(top, f_top, preferred_element_type=jnp.float32)
    weighted += jnp.dot(low, f_top, preferred_element_type=jnp.float32)
    weighted += jnp.dot(top, f_low, preferred_element_type=jnp.float32)
    return jnp.sum(a_ref[...] * weighted, axis=0, keepdims=True)


def fill_table(raw_ref, tab_ref, chunks, read):
    for chunk in range(chunks):
        for number in range(6):
            line = 48 * chunk + 8 * number
            raw_ref[line : line + 8, :] = read(number, chunk)
    top, low = halves(raw_ref[...])
    tab_ref[:, :LANES] = top
    tab_ref[:, LANES:] = low


def lookup(tab_ref, rows, first, last, olds=(None, None)):
    hot = jnp.concatenate([one_hot(row & (LANES - 1)) for row in rows], axis=1)
    found = jnp.dot(tab_ref[...], jnp.concatenate([hot, hot], axis=0), preferred_element_type=jnp.float32)
    results = []
    for place, (row, old) in enumerate(zip(rows, olds)):
        hi = jnp.broadcast_to(row >> 7, (8, LANES))
        got = [None] * 6 if old is None else old
        for chunk in range(first, last):
            base = 48 * (chunk - first)
            new = [found[base + 8 * r : base + 8 * r + 8, place * LANES : (place + 1) * LANES] for r in range(6)]
            here = hi == chunk
            got = [fresh if kept is None else jnp.where(here, fresh, kept) for fresh, kept in zip(new, got)]
        results.append(got)
    return results


def lines(corner):
    return [(8 * comp + corner) * 8 for comp in range(3)]


def put(f_ref, a_ref, corner, cols, got):
    for comp, line in enumerate(lines(corner)):
        f_ref[line : line + 8, cols] = got[comp]
        a_ref[line : line + 8, cols] = got[3 + comp]


def own_corners(tab_ref, nodes, elem, pairs, lone, f_ref, a_ref, cols):
    for pair in pairs:
        for corner, got in zip(pair, lookup(tab_ref, [elem[n : n + 1] for n in pair], 0, OWN_CHUNKS)):
            put(f_ref, a_ref, corner, cols, got)
    for corner in lone:
        lo, hi = split_index(elem[corner : corner + 1])
        put(f_ref, a_ref, corner, cols, select_rows(nodes, lo, hi, OWN_CHUNKS))


def ghost_corners(tab_ref, elem, first, last, old_f, old_a, f_ref, a_ref, cols, fresh):
    for pair in range(4):
        corners = (2 * pair, 2 * pair + 1)
        olds = [
            None
            if corner == 0 and fresh
            else [ref[line : line + 8, cols] for ref in (old_f, old_a) for line in lines(corner)]
            for corner in corners
        ]
        for corner, got in zip(corners, lookup(tab_ref, [elem[n : n + 1] for n in corners], first, last, olds)):
            put(f_ref, a_ref, corner, cols, got)


SOURCES = 12


def pack_kernel(*refs):
    sources, outs, (raw_s, sn_ref, sem) = refs[:SOURCES], refs[SOURCES:-3], refs[-3:]
    far_ref, near_refs, cells_ref, faces_ref = outs[0], outs[1 : NEAR + 1], outs[NEAR + 1], outs[NEAR + 2]
    tab_ref, local = outs[NEAR + 3], (*outs[NEAR + 4 :], sn_ref)
    copies = [pltpu.make_async_copy(far, near, sem.at[n]) for n, (far, near) in enumerate(zip(sources, local))]
    for copy in copies:
        copy.start()
    for copy in (*copies[:4], copies[-1]):
        copy.wait()
    p_ref, q_ref, k_ref, cf_ref, sc_ref, d_ref, a_ref = local[:7]
    nodes = node_tables(d_ref, a_ref)
    cells = cell_tables(p_ref, q_ref)
    perm = [k_ref[0:8, :], k_ref[8:16, :]]
    for m in range(FX // LANES):
        cols = slice(m * LANES, (m + 1) * LANES)
        lo, hi = split_index(cf_ref[0:1, cols])
        pa, qa = select_rows(cells, lo, hi, OWN_CHUNKS)
        ka = select_scalar(perm, lo, hi)
        slot = cf_ref[1:2, cols].astype(jnp.float32)
        for ref, base in [(one, FACE_ROW) for one in near_refs] + [(faces_ref, 0), (far_ref, FAR_FACES)]:
            ref[base + 16 * m : base + 16 * m + 8, :] = pa
            ref[base + 16 * m + 8 : base + 16 * m + 16, :] = qa
            ref[base + 128 + m : base + 129 + m, :] = ka
            ref[base + 136 + m : base + 137 + m, :] = slot
    for copy in copies[4:7]:
        copy.wait()
    fill_table(raw_s, tab_ref, OWN_CHUNKS, lambda number, chunk: nodes[number](chunk))
    for j in range(SLOTS):
        out, start = (near_refs[ORDER.index(j)], 0) if j < NEAR else (far_ref, BLOCK * (j - NEAR))
        if j % 2 == 0:
            both = lookup(tab_ref, [sn_ref[n : n + 1, :] for n in (j, j + 1)], 0, OWN_CHUNKS)
        for number, value in enumerate(both[j % 2]):
            out[start + 8 * number : start + 8 * number + 8, :] = value
        lo, hi = split_index(sc_ref[j : j + 1, :])
        pb, qb = select_rows(cells, lo, hi, OWN_CHUNKS)
        kb = jnp.broadcast_to(select_scalar(perm, lo, hi), (8, LANES))
        for ref, base in ((out, start + NODE_ROWS), (cells_ref, 24 * j)):
            ref[base : base + 8, :] = pb
            ref[base + 8 : base + 16, :] = qb
            ref[base + 16 : base + 24, :] = kb
    for copy in copies[7:-1]:
        copy.wait()


FACE_BLOCK = 6
EARLY = FI // FACE_BLOCK
ORDER = (3, 5, 1, 0, 4, 2)
NEAR = len(ORDER)
BLOCK = NODE_ROWS + 24
FAR_FACES = 2 * BLOCK
FAR_ROWS = FAR_FACES + 144


AHEAD = 4
WIDTH = FACE_BLOCK * LANES


def steps_ahead():
    return jnp.where((lax.axis_index("dom") & 8) == 0, AHEAD, 0)


def early_steps(first, last, total, tab_ref, p_ref, q_ref, k_ref, en_ref, if_ref, f_s, a_s, t_s):
    cells = cell_tables(p_ref, q_ref)
    perm = [k_ref[0:8, :], k_ref[8:16, :]]
    before = pl.multiple_of(jnp.maximum(first - 1, 0) * WIDTH, WIDTH)
    t_s[:, pl.ds(before, WIDTH)] = jnp.zeros((2, WIDTH), jnp.float32)

    def add(step, total):
        cols = pl.ds(pl.multiple_of(step * WIDTH, WIDTH), WIDTH)
        for side in range(2):
            total = total + scatter(if_ref[side : side + 1, cols], t_s[side : side + 1, cols])
        return total

    def block(step, total):
        total = add(jnp.maximum(step - 1, 0), total)
        cols = pl.ds(pl.multiple_of(step * LANES, LANES), LANES)
        elem = en_ref[:, cols]
        own_corners(tab_ref, None, elem, ((0, 1), (2, 3), (4, 5), (6, 7)), (), f_s, a_s, cols)
        for face in range(FACE_BLOCK):
            offset = pl.multiple_of(step * WIDTH + face * LANES, LANES)
            ends = []
            for side in range(2):
                lo, hi = split_index(if_ref[side : side + 1, pl.ds(offset, LANES)])
                ends += select_rows(cells, lo, hi, OWN_CHUNKS) + [select_scalar(perm, lo, hi)]
            term_a, term_b = face_terms(*ends)
            t_s[0:1, pl.ds(offset, LANES)] = term_a
            t_s[1:2, pl.ds(offset, LANES)] = term_b
        return total

    return add(last - 1, lax.fori_loop(first, last, block, total))


def ahead_kernel(tab_ref, p_ref, q_ref, k_ref, y_ref, s_ref, en_ref, if_ref, gy_ref, gp_ref, f_s, a_s, t_s):
    zero = jnp.zeros((OWN_CHUNKS, LANES), jnp.float32)
    gp_ref[...] = zero
    gy_ref[...] = jnp.zeros((1, AHEAD * LANES), jnp.float32)

    @pl.when(steps_ahead() > 0)
    def _():
        gp_ref[...] = early_steps(0, AHEAD, zero, tab_ref, p_ref, q_ref, k_ref, en_ref, if_ref, f_s, a_s, t_s)
        gy_ref[...] = -y_ref[:, : AHEAD * LANES] * strain_of(s_ref, f_s, a_s)


def inner_kernel(
    tab_ref, d_ref, a_ref, p_ref, q_ref, k_ref, y_ref, s_ref, en_ref, if_ref, gya_ref, gpa_ref,
    gy_ref, gp_ref, fo_ref, ao_ref, f_s, a_s, t_s,
):
    nodes = node_tables(d_ref, a_ref)
    first = steps_ahead()
    gp_ref[...] = early_steps(
        first, FI // WIDTH, gpa_ref[...], tab_ref, p_ref, q_ref, k_ref, en_ref, if_ref, f_s, a_s, t_s
    )

    def late(step, _):
        start = pl.multiple_of(step * LANES, LANES)
        place = pl.multiple_of(EARLY + start, LANES)
        elem = en_ref[:, pl.ds(place, LANES)]
        own_corners(tab_ref, nodes, elem, ((0, 1), (2, 3), (4, 5)), (6, 7), f_s, a_s, pl.ds(place, LANES))
        elem = en_ref[:, pl.ds(pl.multiple_of(OWN + start, LANES), LANES)]
        own_corners(tab_ref, nodes, elem, ((1, 2), (3, 4)), (5, 6, 7), fo_ref, ao_ref, pl.ds(start, LANES))
        return 0

    lax.fori_loop(0, EB // LANES, late, 0)
    gy_ref[...] = -y_ref[:, :OWN] * strain_of(s_ref, f_s, a_s)

    @pl.when(first > 0)
    def _():
        gy_ref[:, : AHEAD * LANES] = gya_ref[...]


def incoming(got, cells_ref, sc_ref, slots, i_s, t_s, start):
    for number, j in enumerate(slots):
        mine = j ^ 1
        pt = cells_ref[24 * mine : 24 * mine + 8, :]
        qt = cells_ref[24 * mine + 8 : 24 * mine + 16, :]
        kt = cells_ref[24 * mine + 16 : 24 * mine + 24, :]
        place = jnp.broadcast_to(sc_ref[mine : mine + 1, :], (8, LANES))
        for m in range(FX // LANES):
            base = start + number * FX + m * LANES
            cols = slice(base, base + LANES)
            lo, hi = split_index(got[j][FACE_ID + m : FACE_ID + m + 1, :].astype(jnp.int32))
            pa = got[j][FACE_ROW + 16 * m : FACE_ROW + 16 * m + 8, :]
            qa = got[j][FACE_ROW + 16 * m + 8 : FACE_ROW + 16 * m + 16, :]
            ka = got[j][FACE_K + m : FACE_K + m + 1, :]
            kb = lane_take(kt, lo)[0:1]
            term = face_terms(pa, qa, ka, lane_take(pt, lo), lane_take(qt, lo), kb)[1]
            i_s[0:1, cols] = lane_take(place, lo)[0:1]
            t_s[0:1, cols] = jnp.where(hi[0:1] == mine, term, 0.0)


def add_terms(i_s, t_s, count, total):
    def add(step, total):
        cols = pl.ds(pl.multiple_of(step * 1024, 1024), 1024)
        return total + scatter(i_s[0:1, cols], t_s[0:1, cols])

    return lax.fori_loop(0, count, add, total)


def tail_kernel(*refs):
    near, (swapped, relayed) = refs[:NEAR], refs[NEAR : NEAR + 2]
    (fo_ref, ao_ref, cells_ref, faces_ref, y_ref, s_ref, sc_ref, en_ref, cf_ref, gyi_ref, gpi_ref) = refs[NEAR + 2 : NEAR + 13]
    gy_ref, gp_ref, f_s, a_s, i_s, t_s, raw_s, tab_s, up_s, down_s = refs[NEAR + 13 :]
    got = [near[ORDER.index(j)] for j in range(NEAR)] + [up_s, down_s]
    low = jnp.broadcast_to((lax.axis_index("dom") & 8) == 0, (8, LANES))
    for ref, start, direct, other in ((up_s, 0, swapped, relayed), (down_s, BLOCK, relayed, swapped)):
        for to, source, length in ((0, start, BLOCK), (BLOCK, FAR_FACES, 144)):
            for row in range(0, length, 8):
                ref[to + row : to + row + 8, :] = jnp.where(
                    low, direct[source + row : source + row + 8, :], other[source + row : source + row + 8, :]
                )
    fill_table(raw_s, tab_s, SLOTS, lambda number, chunk: got[chunk][8 * number : 8 * number + 8, :])
    for step in range(EB // LANES):
        elem = en_ref[:, OWN + step * LANES : OWN + (step + 1) * LANES]
        cols = slice(step * LANES, (step + 1) * LANES)
        ghost_corners(tab_s, elem, OWN_CHUNKS, OWN_CHUNKS + SLOTS, fo_ref, ao_ref, f_s, a_s, cols, True)

    ghosts = [
        lambda h: got[h][NODE_ROWS : NODE_ROWS + 8, :],
        lambda h: got[h][NODE_ROWS + 8 : NODE_ROWS + 16, :],
    ]
    ghost_perm = jnp.concatenate([got[j][NODE_ROWS + 16 : NODE_ROWS + 17, :] for j in range(SLOTS)], axis=0)
    for m in range(FX // LANES):
        cols = slice(m * LANES, (m + 1) * LANES)
        lo, hi = split_index(cf_ref[1:2, cols])
        pb, qb = select_rows(ghosts, lo, hi, SLOTS)
        kb = select_scalar([ghost_perm], lo, hi)
        pa = faces_ref[16 * m : 16 * m + 8, :]
        qa = faces_ref[16 * m + 8 : 16 * m + 16, :]
        ka = faces_ref[128 + m : 129 + m, :]
        i_s[0:1, cols] = cf_ref[0:1, cols]
        t_s[0:1, cols] = face_terms(pa, qa, ka, pb, qb, kb)[0]
    incoming(got, cells_ref, sc_ref, range(SLOTS), i_s, t_s, FX)
    gp_ref[...] = add_terms(i_s, t_s, SLOTS + 1, gpi_ref[...])
    gy_ref[:, :OWN] = gyi_ref[...]
    gy_ref[:, OWN:] = -y_ref[:, OWN:] * strain_of(s_ref, f_s, a_s)


def shape(*dims):
    return jax.ShapeDtypeStruct(dims, jnp.float32)


def on_device(
    displacement,
    adjoint_disp,
    pressure,
    adjoint_pressure,
    youngs,
    permeability,
    stiffness,
    send_nodes,
    send_cells,
    elem_nodes,
    inner_faces,
    cross_faces,
):
    forward = displacement.transpose(1, 0, 2)
    adjoint = adjoint_disp.transpose(1, 0, 2)
    perm = permeability.reshape(OWN_CHUNKS, LANES)
    young = youngs.reshape(1, EL)
    sources = (
        pressure,
        adjoint_pressure,
        perm,
        cross_faces,
        send_cells,
        forward,
        adjoint,
        elem_nodes,
        inner_faces,
        young,
        stiffness,
        send_nodes,
    )
    packed = pl.pallas_call(
        pack_kernel,
        out_shape=[shape(FAR_ROWS, LANES)]
        + [shape(ROWS, LANES)] * NEAR
        + [shape(24 * SLOTS, LANES), shape(144, LANES)]
        + [jax.ShapeDtypeStruct((48 * OWN_CHUNKS, 2 * LANES), jnp.bfloat16)]
        + [jax.ShapeDtypeStruct(one.shape, one.dtype) for one in sources[:-1]],
        in_specs=[pl.BlockSpec(memory_space=pltpu.HBM)] * SOURCES,
        scratch_shapes=[
            pltpu.VMEM((48 * OWN_CHUNKS, LANES), jnp.float32),
            pltpu.VMEM((SLOTS, LANES), jnp.int32),
            pltpu.SemaphoreType.DMA((SOURCES,)),
        ],
        compiler_params=VMEM,
        name="pack",
    )(*(pltpu.with_memory_space_constraint(one, pltpu.HBM) for one in sources))
    cells, faces, table = packed[NEAR + 1 : NEAR + 4]
    (
        pressure,
        adjoint_pressure,
        perm,
        cross_faces,
        send_cells,
        forward,
        adjoint,
        elem_nodes,
        inner_faces,
        young,
        stiffness,
    ) = packed[NEAR + 4 :]
    count = lax.axis_size("dom")
    ahead_young, ahead_perm = pl.pallas_call(
        ahead_kernel,
        out_shape=[shape(1, AHEAD * LANES), shape(OWN_CHUNKS, LANES)],
        scratch_shapes=[
            pltpu.VMEM((192, AHEAD * LANES), jnp.float32),
            pltpu.VMEM((192, AHEAD * LANES), jnp.float32),
            pltpu.VMEM((2, AHEAD * WIDTH), jnp.float32),
        ],
        compiler_params=VMEM,
        name="ahead",
    )(table, pressure, adjoint_pressure, perm, young, stiffness, elem_nodes, inner_faces)
    blocks = lax.optimization_barrier((*packed[: NEAR + 1], ahead_young, ahead_perm))
    packed, (ahead_young, ahead_perm) = blocks[: NEAR + 1], blocks[NEAR + 1 :]
    swapped = lax.ppermute(packed[0], "dom", [(source, source ^ 8) for source in range(count)])
    near = []
    for number, j in enumerate(ORDER):
        pairs = [(source, (source - OFFSETS[j]) % count) for source in range(count)]
        near.append(lax.ppermute(packed[number + 1], "dom", pairs))
    relayed = lax.ppermute(
        swapped, "dom", [(source, (source - 16 if source & 8 else source + 16) % count) for source in range(count)]
    )
    own_young, own_perm, edge_forward, edge_adjoint = pl.pallas_call(
        inner_kernel,
        out_shape=[shape(1, OWN), shape(OWN_CHUNKS, LANES), shape(192, EB), shape(192, EB)],
        scratch_shapes=[
            pltpu.VMEM((192, OWN), jnp.float32),
            pltpu.VMEM((192, OWN), jnp.float32),
            pltpu.VMEM((2, FI), jnp.float32),
        ],
        compiler_params=VMEM,
        cost_estimate=pl.CostEstimate(flops=4 * 10**9, bytes_accessed=10**7, transcendentals=0),
        name="inner",
    )(table, forward, adjoint, pressure, adjoint_pressure, perm, young, stiffness, elem_nodes, inner_faces, ahead_young, ahead_perm)
    grad_young, grad_perm = pl.pallas_call(
        tail_kernel,
        out_shape=[shape(1, EL), shape(OWN_CHUNKS, LANES)],
        scratch_shapes=[
            pltpu.VMEM((192, EB), jnp.float32),
            pltpu.VMEM((192, EB), jnp.float32),
            pltpu.VMEM((1, (SLOTS + 1) * FX), jnp.int32),
            pltpu.VMEM((1, (SLOTS + 1) * FX), jnp.float32),
            pltpu.VMEM((48 * SLOTS, LANES), jnp.float32),
            pltpu.VMEM((48 * SLOTS, 2 * LANES), jnp.bfloat16),
            pltpu.VMEM((ROWS, LANES), jnp.float32),
            pltpu.VMEM((ROWS, LANES), jnp.float32),
        ],
        compiler_params=VMEM,
        name="tail",
    )(
        *near,
        swapped,
        relayed,
        edge_forward,
        edge_adjoint,
        cells,
        faces,
        young,
        stiffness,
        send_cells,
        elem_nodes,
        cross_faces,
        own_young,
        own_perm,
    )
    return (grad_young.reshape(EL), grad_perm.reshape(EL))


def solution(mesh):
    in_specs = (
        P(None, None, "dom"),
        P(None, None, "dom"),
        P(None, "dom"),
        P(None, "dom"),
        P("dom"),
        P("dom"),
        P(),
        P(None, "dom"),
        P(None, "dom"),
        P(None, "dom"),
        P(None, "dom"),
        P(None, "dom"),
    )
    out_specs = (P("dom"), P("dom"))
    return jax.shard_map(
        on_device, mesh=mesh, in_specs=in_specs, out_specs=out_specs, check_vma=False
    )
```
